256 devices in a mesh: rep: 2 (over z), grp: 8 (over x), tp: 16 (over y, core).
Axes of the slice: x: 8, y: 8, z: 2, core: 2. Of those that a mesh axis runs over, the one named last changes fastest.
The devices are a block of a 8x8x16 slice.
Arguments:
- queries: bfloat16 [1024, 8192], P(('rep', 'grp'), 'tp'), parts along dimension 0, may hold values from -256 to 256
- newest_key_value: bfloat16 [1024, 2, 1024], P(('rep', 'grp')), parts along dimension 0, may hold values from -6 to 6
- kv_pages: bfloat16 [1024, 2, 128, 1024], P(('rep', 'grp', 'tp')), parts along dimension 0, may hold values from -8 to 8
- fetch_slots: int32 [16, 128, 2], P('rep', ('grp', 'tp')), parts along dimension 0, may hold values from -1 to 3, as said below
- block_table: int32 [1024, 8], P(('rep', 'grp')), parts along dimension 0, may hold values from 0 to 255, as said below
- prefix_len: int32 [1024], P(('rep', 'grp')), parts along dimension 0, may hold values from 2 to 1024
- out_weight: bfloat16 [8192, 8192], P('tp'), may hold values from -0.09375 to 0.09375
Outputs:
- attended: bfloat16 [1024, 8192], P(('rep', 'grp'), 'tp'), parts along dimension 0
The draws below stay inside these ranges and needn't reach their ends.
There are 2 independent parts, one for each index of `rep`. The reference program is written for one: setup_inputs(seed, part) draws one part's arguments, and reference() takes and returns one part's arrays. A program takes and returns all parts, laid end to end along the dimension named above; an argument that names none is the same for every part. Nothing has to cross between parts.
Inputs may be any that keep to these rules, and one draw needn't show every extreme that they name: `fetch_slots`: entries of one (group, owner device) are distinct pages of that device's storage; each group takes at most 2 pages from one device, and in every draw some group takes exactly 2 from some device; -1 marks an unused entry, and used entries come first. `block_table`: every entry names a used entry of its group's fetch_slots; requests of a group share their first pages to a varying depth.
All inputs are finite; a program needn't handle non-finite values.
Results may differ from the reference program's by a relative error of at most 0.0057.
Values may be sent and summed in bfloat16 or wider, within the bound.
No kernel may reach another device: no remote copies, remote signals or barrier semaphores. Data moves between devices by JAX's collectives and lax.ppermute only.
A program may use at most 128 MiB of HBM per device.

```python
import math
import jax
import jax.numpy as jnp
from jax import lax

D = 8192
QUERY_HEADS = 64
KEY_VALUE_HEADS = 8
HEAD_SIZE = 128
PAGE_TOKENS = 128
PAGE_LIST_LENGTH = 8
GROUP_PAGE_LIMIT = 2
REQ_GRP = 64
PAGES_DEV = 4
OWNERS = 128
TOTAL_PAGES = 512
SLOTS = 256
TOTAL_REQUESTS = 512
N_GRP = 8


def fetch_plan(key):
    base = jax.random.fold_in(key, 101)
    hot_owner = jax.random.randint(jax.random.fold_in(base, 1), (OWNERS,), 0, 4) == 0
    counts = jax.random.randint(jax.random.fold_in(base, 2), (N_GRP, OWNERS), 0, GROUP_PAGE_LIMIT + 1)
    counts = jnp.where(hot_owner[None, :], GROUP_PAGE_LIMIT, counts)
    forced = jnp.arange(N_GRP) * 7 % OWNERS
    counts = counts.at[jnp.arange(N_GRP), forced].set(GROUP_PAGE_LIMIT)
    perm_keys = jax.random.split(jax.random.fold_in(base, 3), N_GRP * OWNERS)
    perms = jax.vmap(lambda one_key: jax.random.permutation(one_key, PAGES_DEV)[:GROUP_PAGE_LIMIT])(perm_keys)
    perms = perms.reshape(N_GRP, OWNERS, GROUP_PAGE_LIMIT)
    filled = jnp.arange(GROUP_PAGE_LIMIT)[None, None, :] < counts[..., None]
    slots = jnp.where(filled, perms, -1).astype(jnp.int32)
    return (slots, filled)


def page_table(key):
    slots, filled = fetch_plan(key)
    flags = filled.reshape(N_GRP, SLOTS).astype(jnp.int32)
    order = jnp.argsort(1 - flags, axis=1, stable=True).astype(jnp.int32)
    count = jnp.sum(flags, axis=1)
    base = jax.random.fold_in(key, 202)
    group_of = jnp.arange(TOTAL_REQUESTS) // REQ_GRP
    shared_pick = jax.random.randint(jax.random.fold_in(base, 1), (N_GRP, PAGE_LIST_LENGTH), 0, 1 << 20) % count[:, None]
    own_pick = jax.random.randint(jax.random.fold_in(base, 2), (TOTAL_REQUESTS, PAGE_LIST_LENGTH), 0, 1 << 20) % count[group_of][:, None]
    depth = jax.random.randint(jax.random.fold_in(base, 3), (TOTAL_REQUESTS,), 0, PAGE_LIST_LENGTH + 1)
    pick = jnp.where(jnp.arange(PAGE_LIST_LENGTH)[None, :] < depth[:, None], shared_pick[group_of], own_pick)
    return jnp.take_along_axis(order[group_of], pick, axis=1).astype(jnp.int32)


def key_couples(key):
    first_index = jax.random.normal(jax.random.fold_in(key, 404), (TOTAL_PAGES, 2, KEY_VALUE_HEADS * HEAD_SIZE), jnp.float32)
    return jnp.clip(first_index, -6.0, 6.0)


def draw_fetch_slots(key, part):
    return fetch_plan(key)[0]


def draw_block_table(key, part):
    return page_table(key)


def draw_kv_pages(key, part):
    remaining_rows = jax.random.normal(jax.random.fold_in(key, 505), (TOTAL_PAGES, 2, PAGE_TOKENS, KEY_VALUE_HEADS * HEAD_SIZE), jnp.float32)
    remaining_rows = jnp.clip(remaining_rows, -6.0, 6.0)
    remaining_rows = remaining_rows.at[:, 0, 0:2].set(key_couples(key))
    return remaining_rows.astype(jnp.bfloat16)


def draw_queries(key, part):
    drawn = jax.random.normal(jax.random.fold_in(key, 606), (TOTAL_REQUESTS, QUERY_HEADS * HEAD_SIZE), jnp.float32)
    drawn = jnp.clip(drawn, -6.0, 6.0)
    return drawn.astype(jnp.bfloat16)


def place_ends(values, own_key, least, high):
    index_at = [jax.random.randint(jax.random.fold_in(own_key, axis), (), 0, length) for axis, length in enumerate(values.shape)]
    longest = values.shape.index(max(values.shape))
    neighbour = index_at[:longest] + [(index_at[longest] + 1) % values.shape[longest]] + index_at[longest + 1:]
    return values.at[tuple(index_at)].set(least).at[tuple(neighbour)].set(high)


def strengthened(result, stream_key, source, target, parts, factor):
    owner, partner = [(jnp.arange(result.shape[axis_at]) // (result.shape[axis_at] // parts)).reshape([-1 if axis == axis_at else 1 for axis in range(result.ndim)]) for axis_at in (source, target)]
    chosen = jax.random.permutation(stream_key, parts)[partner]
    strong = (owner == chosen) | (owner == (partner + parts // 2) % parts)
    return jnp.where(strong, factor * result, result)


def level_of(own_key, dims, shards, smallest, largest):
    level, own = 1.0, jax.random.fold_in(own_key, 6)
    for dim, parts in shards:
        steps = jnp.exp(jax.random.uniform(jax.random.fold_in(own, dim), (parts,), jnp.float32, smallest / len(shards), largest / len(shards)))
        level = level * jnp.repeat(steps, dims[dim] // parts).reshape([-1 if axis == dim else 1 for axis in range(len(dims))])
    return level


def gaussian(key, shape, deviation, limit, cuts=(), held_as=jnp.bfloat16):
    values = jax.random.normal(key, shape, jnp.float32) * deviation
    if len(cuts) > 0:
        values = level_of(key, shape, cuts, -0.22, 0.18) * values
    return jnp.clip(values, min=-limit, max=limit).astype(held_as)


def heavy_noise(stream_key, dims, spread, bound, cuts, heavy, kind=jnp.bfloat16):
    entries = spread * jax.random.normal(stream_key, dims, jnp.float32)
    if cuts:
        entries = entries * level_of(stream_key, dims, cuts, -0.22, 0.18)
    return jnp.clip(strengthened(entries, jax.random.fold_in(stream_key, 3), *heavy), -bound, bound).astype(kind)


def setup_inputs(seed: int = 0, part: int = 0) -> dict:
    keys = jax.random.split(jax.random.key(seed), 8)
    part_splits = jax.random.split(jax.random.fold_in(keys[7], part), 8)
    queries = draw_queries(jax.random.fold_in(jax.random.fold_in(keys[7], part), 71), part)
    newest_key_value = gaussian(part_splits[1], (TOTAL_REQUESTS, 2, KEY_VALUE_HEADS * HEAD_SIZE), 1.0, 6.0, ((0, 8),))
    kv_pages = draw_kv_pages(jax.random.fold_in(jax.random.fold_in(keys[7], part), 71), part)
    fetch_slots = draw_fetch_slots(jax.random.fold_in(jax.random.fold_in(keys[7], part), 71), part)
    block_table = draw_block_table(jax.random.fold_in(jax.random.fold_in(keys[7], part), 71), part)
    prefix_len = place_ends(jax.random.randint(part_splits[5], (TOTAL_REQUESTS,), 2, PAGE_LIST_LENGTH * PAGE_TOKENS + 1), jax.random.fold_in(part_splits[5], 1), 2, PAGE_LIST_LENGTH * PAGE_TOKENS).astype(jnp.int32)
    out_weight = heavy_noise(keys[6], (QUERY_HEADS * HEAD_SIZE, D), (QUERY_HEADS * HEAD_SIZE) ** -0.5, 0.09375, ((0, 16),), (0, 1, 16, 2.0))
    return dict(queries=queries, newest_key_value=newest_key_value, kv_pages=kv_pages, fetch_slots=fetch_slots, block_table=block_table, prefix_len=prefix_len, out_weight=out_weight)


def reference(queries, newest_key_value, kv_pages, fetch_slots, block_table, prefix_len, out_weight):
    group_width = QUERY_HEADS // KEY_VALUE_HEADS
    group_of = (jnp.arange(TOTAL_REQUESTS) // REQ_GRP).astype(jnp.int32)
    page_owner = (block_table // GROUP_PAGE_LIMIT).astype(jnp.int32)
    column = (block_table % GROUP_PAGE_LIMIT).astype(jnp.int32)
    stored = fetch_slots[group_of[:, None], page_owner, column]
    page_index = (page_owner * PAGES_DEV + stored).astype(jnp.int32)
    score_scale = 1.0 / math.sqrt(HEAD_SIZE)

    def single(inputs):
        query_vector, newest_token, pages_used, length = inputs
        chosen_pages = kv_pages[pages_used]
        key_matrix = chosen_pages[:, 0].reshape(PAGE_LIST_LENGTH * PAGE_TOKENS, KEY_VALUE_HEADS, HEAD_SIZE).astype(jnp.float32)
        value_matrix = chosen_pages[:, 1].reshape(PAGE_LIST_LENGTH * PAGE_TOKENS, KEY_VALUE_HEADS, HEAD_SIZE).astype(jnp.float32)
        head_list = query_vector.reshape(KEY_VALUE_HEADS, group_width, HEAD_SIZE).astype(jnp.float32)
        newest_rows = newest_token.reshape(2, KEY_VALUE_HEADS, HEAD_SIZE).astype(jnp.float32)
        scores = jnp.einsum('kqd,pkd->kqp', head_list, key_matrix) * score_scale
        live_mask = jnp.arange(PAGE_LIST_LENGTH * PAGE_TOKENS) < length
        scores = jnp.where(live_mask[None, None, :], scores, -jnp.inf)
        own_score = jnp.einsum('kqd,kd->kq', head_list, newest_rows[0]) * score_scale
        row_top = jnp.maximum(lax.optimization_barrier(jnp.max(scores, axis=-1)), own_score)
        exp_terms = jnp.exp(scores - row_top[..., None])
        exp_own = jnp.exp(own_score - row_top)
        denom_sum = lax.optimization_barrier(jnp.sum(exp_terms, axis=-1)) + exp_own
        weights = (exp_terms / denom_sum[..., None]).astype(jnp.bfloat16).astype(jnp.float32)
        weight_own = (exp_own / denom_sum).astype(jnp.bfloat16).astype(jnp.float32)
        mixed = jnp.einsum('kqp,pkd->kqd', weights, value_matrix)
        mixed = mixed + weight_own[..., None] * newest_rows[1][:, None, :]
        return mixed.astype(jnp.bfloat16).reshape(QUERY_HEADS * HEAD_SIZE)
    mix = lax.map(single, (queries, newest_key_value, page_index, prefix_len))
    return jnp.dot(mix, out_weight, preferred_element_type=jnp.float32).astype(jnp.bfloat16)
```

```python
import math

import jax
import jax.numpy as jnp
from jax import lax
from jax.experimental import pallas as pl
from jax.experimental.pallas import tpu as pltpu
from jax.sharding import PartitionSpec as P

HEAD_SIZE = 128
PAGE_TOKENS = 128
META_ROWS = 16
LOW = -1e30
CHUNKS = ((0, 1, 7), (2, 6), (3, 5), (4,))
BATCH = 4
INTERPRET = False


def split3(x):
    hi = x.astype(jnp.bfloat16)
    rest = x - hi.astype(jnp.float32)
    mid = rest.astype(jnp.bfloat16)
    low = (rest - mid.astype(jnp.float32)).astype(jnp.bfloat16)
    return [part.astype(jnp.float32) for part in (hi, mid, low)]


def attend_chunk(pages_of, place, bufs, queries_t, state, shifts, y_count, group_count, pages_dev, first, last):
    n_buf = len(bufs)
    rows = queries_t.shape[1]
    cols = queries_t.shape[2]
    limit = 2 * n_buf
    factor = math.log2(math.e) / math.sqrt(HEAD_SIZE)

    def kernel(pages_ref, place_ref, *refs):
        buf_refs = refs[:n_buf]
        q_ref = refs[n_buf]
        rest = refs[n_buf + 1 :]
        if not first:
            acc_in, ml_in, *rest = rest
        if last:
            out_ref, *rest = rest
            acc, ml, store, item_page, item_slot, sem = rest
        else:
            acc, ml, store, item_page, item_slot, sem = rest
        g = pl.program_id(0)
        copies = [pltpu.make_async_copy(buf_refs[b], store.at[b], sem.at[b]) for b in range(n_buf)]

        @pl.when(g == 0)
        def _():
            for one in copies:
                one.start()

        tp_rank = place_ref[0]
        row = place_ref[1]
        core = tp_rank % 2
        count = jnp.int32(0)
        for b in range(n_buf):
            source_y = (tp_rank // 2 + y_count - shifts[b // 2]) % y_count
            owner = 2 * source_y + (core if b % 2 == 0 else 1 - core)
            for column in range(2):
                page = pages_ref[(owner * group_count + g) * 2 + column]
                item_page[count] = b * pages_dev + page
                item_slot[count] = (row * 2 * y_count + owner) * 2 + column
                count = count + jnp.where(page >= 0, 1, 0)
        for pad in range(BATCH):
            item_page[count + pad] = 0
            item_slot[count + pad] = -1

        if first:
            acc[0] = jnp.zeros(acc.shape[1:], jnp.float32)
            ml[0] = jnp.where(lax.broadcasted_iota(jnp.int32, ml.shape[1:], 0) == 0, LOW, 0.0)
        else:
            acc[0] = acc_in[0]
            ml[0] = ml_in[0]

        @pl.when(g == 0)
        def _():
            for one in copies:
                one.wait()

        table = q_ref[0, HEAD_SIZE : HEAD_SIZE + 16].astype(jnp.float32)
        length = table[8:9] * 8.0 + table[9:10]
        table = table[0:8]
        entry = lax.broadcasted_iota(jnp.int32, (8, cols), 0).astype(jnp.float32)
        live = jnp.clip(length - PAGE_TOKENS * entry, 0.0, 1.0 * PAGE_TOKENS)
        whole = live == PAGE_TOKENS
        token = lax.broadcasted_iota(jnp.int32, (PAGE_TOKENS, cols), 0).astype(jnp.float32)

        def batch(i, _):
            query = q_ref[0, 0:HEAD_SIZE]
            old = ml[0, 0:1]
            top = old
            scores, counts = [], []
            for j in range(BATCH):
                page = item_page[i * BATCH + j]
                slot = item_slot[i * BATCH + j].astype(jnp.float32)
                key = store[page // pages_dev, page % pages_dev, 0]
                score = jnp.dot(key, query, preferred_element_type=jnp.float32) * factor
                match = table == slot
                full = jnp.sum(jnp.where(match & whole, 1.0, 0.0), axis=0, keepdims=True)
                part = jnp.max(jnp.where(match & ~whole, live, 0.0), axis=0, keepdims=True)
                reach = jnp.where(full > 0.0, 1.0 * PAGE_TOKENS, part)
                score = jnp.where(token < reach, score, LOW)
                top = jnp.maximum(top, jnp.max(score, axis=0, keepdims=True))
                scores.append(score)
                counts.append((full, part))
            shrink = jnp.exp2(old - top)
            total = ml[0, 1:2] * shrink
            update = acc[0] * shrink
            for j in range(BATCH):
                page = item_page[i * BATCH + j]
                full, part = counts[j]
                weight = jnp.exp2(scores[j] - top) * jnp.where(token < part, full + 1.0, full)
                total = total + jnp.sum(weight, axis=0, keepdims=True)
                value = store[page // pages_dev, page % pages_dev, 1]
                update = update + lax.dot_general(
                    value, weight.astype(jnp.bfloat16), (((0,), (0,)), ((), ())), preferred_element_type=jnp.float32
                )
            acc[0] = update
            ml[0, 0:1] = top
            ml[0, 1:2] = total
            return 0

        lax.fori_loop(0, (count + BATCH - 1) // BATCH, batch, 0)

        if last:
            top = ml[0, 0:1]
            total = ml[0, 1:2]
            inverse = jnp.where(total > 0.0, 1.0 / jnp.where(total > 0.0, total, 1.0), 0.0)
            out_ref[0, 0:HEAD_SIZE] = (acc[0] * inverse).astype(jnp.bfloat16)
            sub = lax.broadcasted_iota(jnp.int32, (META_ROWS, cols), 0)
            packed = jnp.zeros((META_ROWS, cols), jnp.float32)
            for n, part in enumerate(split3(top) + split3(total)):
                packed = jnp.where(sub == n, part, packed)
            out_ref[0, HEAD_SIZE:] = packed.astype(jnp.bfloat16)

    def block(*shape):
        return pl.BlockSpec((1,) + shape, lambda g, *_: (g,) + (0,) * len(shape))

    acc_shape = jax.ShapeDtypeStruct((group_count, HEAD_SIZE, cols), jnp.float32)
    ml_shape = jax.ShapeDtypeStruct((group_count, 8, cols), jnp.float32)
    state_specs = [block(HEAD_SIZE, cols), block(8, cols)]
    scratch = [
        pltpu.VMEM((n_buf, pages_dev, 2, PAGE_TOKENS, HEAD_SIZE), jnp.bfloat16),
        pltpu.SMEM((limit + BATCH,), jnp.int32),
        pltpu.SMEM((limit + BATCH,), jnp.int32),
        pltpu.SemaphoreType.DMA((n_buf,)),
    ]
    in_specs = [pl.BlockSpec(memory_space=pl.ANY)] * n_buf + [block(rows, cols)]
    if not first:
        in_specs = in_specs + state_specs
    if last:
        out_shape = jax.ShapeDtypeStruct((group_count, HEAD_SIZE + META_ROWS, cols), jnp.bfloat16)
        out_specs = block(HEAD_SIZE + META_ROWS, cols)
        scratch = [pltpu.VMEM((1, HEAD_SIZE, cols), jnp.float32), pltpu.VMEM((1, 8, cols), jnp.float32)] + scratch
        aliases = {}
    else:
        out_shape = (acc_shape, ml_shape)
        out_specs = tuple(state_specs)
        aliases = {} if first else {2 + n_buf + 1: 0, 2 + n_buf + 2: 1}
    return pl.pallas_call(
        kernel,
        out_shape=out_shape,
        grid_spec=pltpu.PrefetchScalarGridSpec(
            num_scalar_prefetch=2, grid=(group_count,), in_specs=in_specs, out_specs=out_specs, scratch_shapes=scratch
        ),
        input_output_aliases=aliases,
        interpret=INTERPRET,
        name="attend_" + "_".join(str(s) for s in shifts),
    )(pages_of, place, *bufs, queries_t, *(() if first else state))


def combine(arrived, query_t, newest_t):
    group_count, _, cols = arrived.shape
    factor = math.log2(math.e) / math.sqrt(HEAD_SIZE)

    def kernel(in_ref, q_ref, new_ref, out_ref):
        query = q_ref[0:HEAD_SIZE].astype(jnp.float32)
        own = jnp.sum(query * new_ref[0].astype(jnp.float32), axis=0, keepdims=True) * factor
        top = own
        tops, totals = [], []
        for n in range(group_count):
            packed = in_ref[n, HEAD_SIZE:].astype(jnp.float32)
            tops.append(packed[0:1] + packed[1:2] + packed[2:3])
            totals.append(packed[3:4] + packed[4:5] + packed[5:6])
            top = jnp.maximum(top, tops[-1])
        own_weight = jnp.exp2(own - top)
        denominator = own_weight
        scales = []
        for n in range(group_count):
            scales.append(totals[n] * jnp.exp2(tops[n] - top))
            denominator = denominator + scales[-1]
        inverse = 1.0 / denominator
        mix = new_ref[1].astype(jnp.float32) * (own_weight * inverse)
        for n in range(group_count):
            mix = mix + in_ref[n, 0:HEAD_SIZE].astype(jnp.float32) * (scales[n] * inverse)
        out_ref[...] = mix.astype(jnp.bfloat16)

    return pl.pallas_call(
        kernel,
        out_shape=jax.ShapeDtypeStruct((HEAD_SIZE, cols), jnp.bfloat16),
        interpret=INTERPRET,
        name="combine",
    )(arrived, query_t, newest_t)


def project(core, mix_own, mix_partner, weight_own, weight_partner, y_count, req_rows):
    width = weight_partner.shape[1] // y_count
    depth = weight_own.shape[0]
    heads = depth // HEAD_SIZE

    def kernel(core_ref, own_ref, partner_ref, w_own_ref, w_partner_ref, out_ref):
        total = jnp.zeros((req_rows, width), jnp.float32)
        for mix_ref, w_ref in ((own_ref, w_own_ref), (partner_ref, w_partner_ref)):
            for h in range(heads):
                total = total + lax.dot_general(
                    mix_ref[:, h * req_rows : (h + 1) * req_rows],
                    w_ref[h * HEAD_SIZE : (h + 1) * HEAD_SIZE, :],
                    (((0,), (0,)), ((), ())),
                    preferred_element_type=jnp.float32,
                )
        out_ref[0] = total.astype(jnp.bfloat16)

    cols = mix_own.shape[1]
    mix_spec = pl.BlockSpec((HEAD_SIZE, cols), lambda n, c: (0, 0))
    return pl.pallas_call(
        kernel,
        out_shape=jax.ShapeDtypeStruct((y_count, req_rows, width), jnp.bfloat16),
        grid_spec=pltpu.PrefetchScalarGridSpec(
            num_scalar_prefetch=1,
            grid=(y_count,),
            in_specs=[
                mix_spec,
                mix_spec,
                pl.BlockSpec((depth, width), lambda n, c: (0, 2 * n + c[0])),
                pl.BlockSpec((depth, width), lambda n, c: (0, n)),
            ],
            out_specs=pl.BlockSpec((1, req_rows, width), lambda n, c: (n, 0, 0)),
        ),
        interpret=INTERPRET,
        name="project",
    )(core, mix_own, mix_partner, weight_own, weight_partner)


def per_device(
    queries, newest_key_value, kv_pages, fetch_slots, block_table, prefix_len, out_weight
):
    tp_count = lax.axis_size("tp")
    group_count = lax.axis_size("grp")
    y_count = tp_count // 2
    tp_rank = lax.axis_index("tp").astype(jnp.int32)
    row = lax.axis_index("grp").astype(jnp.int32)
    y = tp_rank // 2
    core = tp_rank % 2
    req_rows = queries.shape[0]
    heads_dev = queries.shape[1] // HEAD_SIZE
    pages_dev = kv_pages.shape[0]
    list_length = block_table.shape[1]
    cols = heads_dev * req_rows
    swap = [(i, i ^ 1) for i in range(tp_count)]

    def moved(x, shift):
        return lax.ppermute(x, "tp", [(i, (i + 2 * shift) % tp_count) for i in range(tp_count)])

    own, partner = {}, {}
    for shift in [s for chunk in CHUNKS for s in chunk]:
        head = (y + shift) % y_count
        piece = lax.dynamic_slice_in_dim(kv_pages, head * HEAD_SIZE, HEAD_SIZE, 3)
        own[shift] = moved(piece, shift) if shift else piece
    for shift in own:
        partner[shift] = lax.ppermute(own[shift], "tp", swap)

    weight_view = out_weight.reshape(out_weight.shape[0], y_count, 2, -1)
    weight_half = lax.dynamic_index_in_dim(weight_view, 1 - core, 2, keepdims=False)
    weight_partner = lax.ppermute(weight_half.reshape(out_weight.shape[0], -1), "tp", swap)

    query_t = jnp.transpose(queries.reshape(req_rows, heads_dev, HEAD_SIZE), (2, 1, 0)).reshape(HEAD_SIZE, cols)
    meta = jnp.concatenate(
        [block_table.T, (prefix_len // 8)[None], (prefix_len % 8)[None], jnp.zeros((META_ROWS - list_length - 2, req_rows), jnp.int32)], axis=0
    )
    meta = jnp.tile(meta.astype(jnp.bfloat16), (1, heads_dev))
    query_t = jnp.concatenate([query_t, meta], axis=0)
    queries_t = lax.all_gather(query_t, "grp", axis=0)

    stored = lax.all_gather(fetch_slots.reshape(-1), "tp", axis=0).reshape(tp_count, group_count, 2)
    small = queries_t[:, HEAD_SIZE:, :req_rows].astype(jnp.int32)
    table_all = small[:, :list_length]
    length_all = small[:, list_length] * 8 + small[:, list_length + 1]
    live = PAGE_TOKENS * jnp.arange(list_length)[None, :, None] < length_all[:, None, :]
    slot_ids = row * (2 * tp_count) + jnp.arange(2 * tp_count)
    named = jnp.any((table_all[:, None] == slot_ids[None, :, None, None]) & live[:, None], axis=(2, 3))
    named = jnp.transpose(named.reshape(group_count, tp_count, 2), (1, 0, 2))
    pages_of = jnp.where(named, stored, -1).reshape(-1)
    place = jnp.stack([tp_rank, row])

    newest = lax.dynamic_slice_in_dim(newest_key_value, y * HEAD_SIZE, HEAD_SIZE, 2)
    newest_t = jnp.tile(jnp.transpose(newest, (1, 2, 0)), (1, 1, heads_dev))

    state = ()
    for n, shifts in enumerate(CHUNKS):
        bufs = [b for s in shifts for b in (own[s], partner[s])]
        state = attend_chunk(
            pages_of, place, bufs, queries_t, state, shifts, y_count, group_count, pages_dev, n == 0, n == len(CHUNKS) - 1
        )
    arrived = lax.all_to_all(state, "grp", split_axis=0, concat_axis=0, tiled=True)

    mix_own = combine(arrived, query_t, newest_t)
    mix_partner = lax.ppermute(mix_own, "tp", swap)
    partial = project(core.reshape(1), mix_own, mix_partner, out_weight, weight_partner, y_count, req_rows)
    same_core = [[2 * i + c for i in range(y_count)] for c in range(2)]
    arrived = lax.all_to_all(partial, "tp", split_axis=0, concat_axis=0, axis_index_groups=same_core, tiled=True)
    return jnp.sum(arrived.astype(jnp.float32), axis=0).astype(jnp.bfloat16)


def solution(mesh):
    in_specs = (
        P(("rep", "grp"), "tp"),
        P(("rep", "grp"), None, None),
        P(("rep", "grp", "tp"), None, None, None),
        P("rep", ("grp", "tp"), None),
        P(("rep", "grp"), None),
        P(("rep", "grp")),
        P("tp", None),
    )
    out_specs = P(("rep", "grp"), "tp")
    return jax.shard_map(
        per_device, mesh=mesh, in_specs=in_specs, out_specs=out_specs, check_vma=False
    )
```

```python
import math

import jax
import jax.numpy as jnp
from jax import lax
from jax.experimental import pallas as pl
from jax.experimental.pallas import tpu as pltpu
from jax.sharding import PartitionSpec as P

HEAD_SIZE = 128
PAGE_TOKENS = 128
META_ROWS = 16
LOW = -1e30
CHUNKS = ((0, 1, 7), (2, 6), (3, 5), (4,))
INTERPRET = False


def split3(x):
    hi = x.astype(jnp.bfloat16)
    rest = x - hi.astype(jnp.float32)
    mid = rest.astype(jnp.bfloat16)
    low = (rest - mid.astype(jnp.float32)).astype(jnp.bfloat16)
    return [part.astype(jnp.float32) for part in (hi, mid, low)]


def attend_chunk(stored, named, place, bufs, queries_t, state, shifts, y_count, group_count, pages_dev, per_batch, first, last):
    n_buf = len(bufs)
    rows, cols = queries_t[0].shape
    limit = 2 * n_buf
    factor = math.log2(math.e) / math.sqrt(HEAD_SIZE)

    def kernel(stored_ref, named_ref, place_ref, *refs):
        buf_refs = refs[:n_buf]
        q_refs = refs[n_buf : n_buf + group_count]
        rest = list(refs[n_buf + group_count :])
        if not first:
            acc_in, ml_in = rest[:2]
            rest = rest[2:]
        if last:
            out_refs = rest[:group_count]
            rest = rest[group_count:]
        else:
            acc_out, ml_out = rest[:2]
            rest = rest[2:]
        acc, ml, store, query_all, out_all, item_page, item_slot, sem_store, sem_query, sem_acc, sem_ml, sem_out = rest
        tp_rank = place_ref[0]
        row = place_ref[1]
        core = lax.rem(tp_rank, 2)

        query_copies = [pltpu.make_async_copy(q_refs[g], query_all.at[g], sem_query.at[g]) for g in range(group_count)]
        store_copies = [pltpu.make_async_copy(buf_refs[b], store.at[b], sem_store.at[b]) for b in range(n_buf)]
        if not first:
            ml_copy = pltpu.make_async_copy(ml_in, ml, sem_ml)
            acc_copies = [pltpu.make_async_copy(acc_in.at[g], acc.at[g], sem_acc.at[g]) for g in range(group_count)]
            ml_copy.start()
        for one in store_copies + query_copies:
            one.start()
        if first:
            acc[...] = jnp.zeros(acc.shape, jnp.float32)
            ml[...] = jnp.where(lax.broadcasted_iota(jnp.int32, ml.shape, 1) == 0, LOW, 0.0)
        else:
            for one in acc_copies:
                one.start()
            ml_copy.wait()
            for one in acc_copies:
                one.wait()
        for one in query_copies + store_copies:
            one.wait()

        entry = lax.broadcasted_iota(jnp.int32, (8, cols), 0).astype(jnp.float32)
        token = lax.broadcasted_iota(jnp.int32, (PAGE_TOKENS, cols), 0).astype(jnp.float32)

        def group(g, _):
            number = lax.rem(row + group_count - g, group_count)
            count = jnp.int32(0)
            for b in range(n_buf):
                source_y = lax.rem(lax.div(tp_rank, 2) + y_count - shifts[b // 2], y_count)
                owner = 2 * source_y + (core if b % 2 == 0 else 1 - core)
                for column in range(2):
                    page = stored_ref[(owner * group_count + number) * 2 + column]
                    slot = (row * 2 * y_count + owner) * 2 + column
                    item_page[count] = b * pages_dev + page
                    item_slot[count] = slot
                    used = named_ref[g * (4 * y_count * group_count) + slot]
                    count = count + jnp.where((page >= 0) & (used > 0), 1, 0)
            for pad in range(per_batch):
                item_page[count + pad] = 0
                item_slot[count + pad] = -1

            table = query_all[g, HEAD_SIZE : HEAD_SIZE + 16].astype(jnp.float32)
            length = table[8:9] * 8.0 + table[9:10]
            table = table[0:8]
            live = jnp.clip(length - PAGE_TOKENS * entry, 0.0, 1.0 * PAGE_TOKENS)
            whole = live == PAGE_TOKENS

            def batch(i, _):
                query = query_all[g, 0:HEAD_SIZE]
                old = ml[g, 0:1]
                top = old
                scores, counts = [], []
                for j in range(per_batch):
                    page = item_page[i * per_batch + j]
                    slot = item_slot[i * per_batch + j].astype(jnp.float32)
                    key = store[lax.div(page, pages_dev), lax.rem(page, pages_dev), 0]
                    score = jnp.dot(key, query, preferred_element_type=jnp.float32) * factor
                    match = table == slot
                    full = jnp.sum(jnp.where(match & whole, 1.0, 0.0), axis=0, keepdims=True)
                    part = jnp.max(jnp.where(match & ~whole, live, 0.0), axis=0, keepdims=True)
                    reach = jnp.where(full > 0.0, 1.0 * PAGE_TOKENS, part)
                    score = jnp.where(token < reach, score, LOW)
                    top = jnp.maximum(top, jnp.max(score, axis=0, keepdims=True))
                    scores.append(score)
                    counts.append((full, part))
                shrink = jnp.exp2(old - top)
                total = ml[g, 1:2] * shrink
                update = acc[g] * shrink
                for j in range(per_batch):
                    page = item_page[i * per_batch + j]
                    full, part = counts[j]
                    weight = jnp.exp2(scores[j] - top) * jnp.where(token < part, full + 1.0, full)
                    total = total + jnp.sum(weight, axis=0, keepdims=True)
                    value = store[lax.div(page, pages_dev), lax.rem(page, pages_dev), 1]
                    update = update + lax.dot_general(
                        value, weight.astype(jnp.bfloat16), (((0,), (0,)), ((), ())), preferred_element_type=jnp.float32
                    )
                acc[g] = update
                ml[g, 0:1] = top
                ml[g, 1:2] = total
                return 0

            lax.fori_loop(0, lax.div(count + per_batch - 1, per_batch), batch, 0)

            if last:
                top = ml[g, 0:1]
                total = ml[g, 1:2]
                inverse = jnp.where(total > 0.0, 1.0 / jnp.where(total > 0.0, total, 1.0), 0.0)
                out_all[g, 0:HEAD_SIZE] = (acc[g] * inverse).astype(jnp.bfloat16)
                sub = lax.broadcasted_iota(jnp.int32, (META_ROWS, cols), 0)
                packed = jnp.zeros((META_ROWS, cols), jnp.float32)
                for n, part in enumerate(split3(top) + split3(total)):
                    packed = jnp.where(sub == n, part, packed)
                out_all[g, HEAD_SIZE:] = packed.astype(jnp.bfloat16)
            return 0

        lax.fori_loop(0, group_count, group, 0)
        if last:
            out_copies = [pltpu.make_async_copy(out_all.at[g], out_refs[g], sem_out.at[g]) for g in range(group_count)]
        else:
            out_copies = [pltpu.make_async_copy(acc.at[g], acc_out.at[g], sem_out.at[g]) for g in range(group_count)]
            out_copies.append(pltpu.make_async_copy(ml, ml_out, sem_ml))
        for one in out_copies:
            one.start()
        for one in out_copies:
            one.wait()

    if last:
        out_shape = [jax.ShapeDtypeStruct((HEAD_SIZE + META_ROWS, cols), jnp.bfloat16)] * group_count
        aliases = {}
    else:
        out_shape = [
            jax.ShapeDtypeStruct((group_count, HEAD_SIZE, cols), jnp.float32),
            jax.ShapeDtypeStruct((group_count, 8, cols), jnp.float32),
        ]
        aliases = {} if first else {3 + n_buf + group_count: 0, 3 + n_buf + group_count + 1: 1}
    n_out_slots = group_count if last else 1
    scratch = [
        pltpu.VMEM((group_count, HEAD_SIZE, cols), jnp.float32),
        pltpu.VMEM((group_count, 8, cols), jnp.float32),
        pltpu.VMEM((n_buf, pages_dev, 2, PAGE_TOKENS, HEAD_SIZE), jnp.bfloat16),
        pltpu.VMEM((group_count, rows, cols), jnp.bfloat16),
        pltpu.VMEM((n_out_slots, HEAD_SIZE + META_ROWS, cols), jnp.bfloat16),
        pltpu.SMEM((limit + per_batch,), jnp.int32),
        pltpu.SMEM((limit + per_batch,), jnp.int32),
        pltpu.SemaphoreType.DMA((n_buf,)),
        pltpu.SemaphoreType.DMA((group_count,)),
        pltpu.SemaphoreType.DMA((group_count,)),
        pltpu.SemaphoreType.DMA,
        pltpu.SemaphoreType.DMA((group_count,)),
    ]
    anywhere = pl.BlockSpec(memory_space=pltpu.MemorySpace.HBM)
    n_in = n_buf + group_count + (0 if first else 2)
    return pl.pallas_call(
        kernel,
        out_shape=out_shape,
        grid_spec=pltpu.PrefetchScalarGridSpec(
            num_scalar_prefetch=3,
            grid=(),
            in_specs=[anywhere] * n_in,
            out_specs=[anywhere] * len(out_shape),
            scratch_shapes=scratch,
        ),
        input_output_aliases=aliases,
        interpret=INTERPRET,
    )(stored, named, place, *bufs, *queries_t, *(() if first else state))


def combine(arrived, query_t, newest_t, heads_dev):
    parts = len(arrived)
    cols = arrived[0].shape[1]
    req_rows = cols // heads_dev
    factor = math.log2(math.e) / math.sqrt(HEAD_SIZE)

    def kernel(*refs):
        in_refs = refs[:parts]
        q_ref, new_ref, out_ref = refs[parts:]
        query = q_ref[0:HEAD_SIZE].astype(jnp.float32)
        own = jnp.sum(query * new_ref[0].astype(jnp.float32), axis=0, keepdims=True) * factor
        top = own
        tops, totals = [], []
        for n in range(parts):
            packed = in_refs[n][HEAD_SIZE:].astype(jnp.float32)
            tops.append(packed[0:1] + packed[1:2] + packed[2:3])
            totals.append(packed[3:4] + packed[4:5] + packed[5:6])
            top = jnp.maximum(top, tops[-1])
        own_weight = jnp.exp2(own - top)
        denominator = own_weight
        scales = []
        for n in range(parts):
            scales.append(totals[n] * jnp.exp2(tops[n] - top))
            denominator = denominator + scales[-1]
        inverse = 1.0 / denominator
        mix = new_ref[1].astype(jnp.float32) * (own_weight * inverse)
        for n in range(parts):
            mix = mix + in_refs[n][0:HEAD_SIZE].astype(jnp.float32) * (scales[n] * inverse)
        for h in range(heads_dev):
            one = mix[:, h * req_rows : (h + 1) * req_rows]
            out_ref[:, h * HEAD_SIZE : (h + 1) * HEAD_SIZE] = one.T.astype(jnp.bfloat16)

    return pl.pallas_call(
        kernel,
        out_shape=jax.ShapeDtypeStruct((req_rows, heads_dev * HEAD_SIZE), jnp.bfloat16),
        interpret=INTERPRET,
        name="combine",
    )(*arrived, query_t, newest_t)


def project(place, mix_own, mix_partner, weight_own, weight_partner, y_count):
    width = weight_own.shape[1] // (2 * y_count)
    req_rows, depth = mix_own.shape

    def kernel(place_ref, own_ref, partner_ref, w_own_ref, w_partner_ref, *out_refs):
        total = jnp.dot(own_ref[...], w_own_ref[...], preferred_element_type=jnp.float32)
        total = total + jnp.dot(partner_ref[...], w_partner_ref[...], preferred_element_type=jnp.float32)
        total = total.astype(jnp.bfloat16)
        for n in range(y_count):

            @pl.when(pl.program_id(0) == n)
            def _():
                out_refs[n][...] = total

    def column(n, place):
        rank = place[0]
        return (0, 2 * lax.rem(lax.div(rank, 2) + n, y_count) + lax.rem(rank, 2))

    mix_spec = pl.BlockSpec((req_rows, depth), lambda n, place: (0, 0))
    return pl.pallas_call(
        kernel,
        out_shape=[jax.ShapeDtypeStruct((req_rows, width), jnp.bfloat16)] * y_count,
        grid_spec=pltpu.PrefetchScalarGridSpec(
            num_scalar_prefetch=1,
            grid=(y_count,),
            in_specs=[mix_spec, mix_spec, pl.BlockSpec((depth, width), column), pl.BlockSpec((depth, width), column)],
            out_specs=[pl.BlockSpec((req_rows, width), lambda n, place: (0, 0))] * y_count,
        ),
        interpret=INTERPRET,
        name="project",
    )(place, mix_own, mix_partner, weight_own, weight_partner)


def per_device_inner(
    queries, newest_key_value, kv_pages, fetch_slots, block_table, prefix_len, out_weight
):
    tp_count = lax.axis_size("tp")
    group_count = lax.axis_size("grp")
    y_count = tp_count // 2
    tp_rank = lax.axis_index("tp").astype(jnp.int32)
    row = lax.axis_index("grp").astype(jnp.int32)
    y = lax.div(tp_rank, 2)
    req_rows = queries.shape[0]
    heads_dev = queries.shape[1] // HEAD_SIZE
    pages_dev = kv_pages.shape[0]
    list_length = block_table.shape[1]
    cols = heads_dev * req_rows
    slots = 2 * tp_count * group_count
    swap = [(i, i ^ 1) for i in range(tp_count)]

    def along_y(x, shift):
        return lax.ppermute(x, "tp", [(i, (i + 2 * shift) % tp_count) for i in range(tp_count)])

    def along_x(x, shift):
        return lax.ppermute(x, "grp", [(i, (i + shift) % group_count) for i in range(group_count)])

    def to_other_core(x):
        return lax.ppermute(x, "tp", swap)

    own, partner = {}, {}
    for shift in [s for chunk in CHUNKS for s in chunk]:
        head = lax.rem(y + shift, y_count)
        piece = lax.dynamic_slice_in_dim(kv_pages, head * HEAD_SIZE, HEAD_SIZE, 3)
        own[shift] = along_y(piece, shift) if shift else piece

    query_t = jnp.transpose(queries.reshape(req_rows, heads_dev, HEAD_SIZE), (2, 1, 0)).reshape(HEAD_SIZE, cols)
    table_t = block_table.T
    live = PAGE_TOKENS * jnp.arange(list_length)[:, None] < prefix_len[None, :]
    alive = jnp.where(live, table_t, -1)
    named = jnp.any(alive[:, :, None] == jnp.arange(slots)[None, None, :], axis=(0, 1)).astype(jnp.bfloat16)
    named = jnp.pad(named, (0, cols - slots))[None]
    meta = jnp.concatenate([table_t, (prefix_len // 8)[None], (prefix_len % 8)[None]], axis=0)
    meta = jnp.tile(meta.astype(jnp.bfloat16), (1, heads_dev))
    fill = jnp.zeros((META_ROWS - list_length - 3, cols), jnp.bfloat16)
    query_t = jnp.concatenate([query_t, meta, named, fill], axis=0)
    queries_t = [along_x(query_t, s) if s else query_t for s in range(group_count)]

    stored = jnp.where(jnp.arange(tp_count)[:, None] == tp_rank, fetch_slots.reshape(1, -1), 0)
    bit = 1
    while bit < tp_count:
        stored = stored + lax.ppermute(stored, "tp", [(i, i ^ bit) for i in range(tp_count)])
        bit *= 2
    stored = stored.reshape(-1)

    for shift in own:
        partner[shift] = to_other_core(own[shift])
    weight_partner = to_other_core(out_weight)

    named_at = HEAD_SIZE + list_length + 2
    named_all = jnp.concatenate([q[named_at : named_at + 1, :slots] for q in queries_t], axis=0)
    named_all = named_all.astype(jnp.int32).reshape(-1)
    place = jnp.stack([tp_rank, row])

    newest = lax.dynamic_slice_in_dim(newest_key_value, y * HEAD_SIZE, HEAD_SIZE, 2)
    newest_t = jnp.tile(jnp.transpose(newest, (1, 2, 0)), (1, 1, heads_dev))

    state = ()
    for n, shifts in enumerate(CHUNKS):
        bufs = [b for s in shifts for b in (own[s], partner[s])]
        last = n == len(CHUNKS) - 1
        state = attend_chunk(
            stored, named_all, place, bufs, queries_t, state, shifts, y_count, group_count, pages_dev, 2 if last else 4, n == 0, last
        )
    arrived = [along_x(state[s], -s) if s else state[s] for s in range(group_count)]

    mix_own = combine(arrived, query_t, newest_t, heads_dev)
    mix_partner = to_other_core(mix_own)
    partial = project(place, mix_own, mix_partner, out_weight, weight_partner, y_count)
    arrived = [along_y(partial[s], s) if s else partial[s] for s in range(y_count)]
    return sum(one.astype(jnp.float32) for one in arrived).astype(jnp.bfloat16)


def solution(mesh):
    in_specs = (
        P(("rep", "grp"), "tp"),
        P(("rep", "grp"), None, None),
        P(("rep", "grp", "tp"), None, None, None),
        P("rep", ("grp", "tp"), None),
        P(("rep", "grp"), None),
        P(("rep", "grp")),
        P("tp", None),
    )
    out_specs = P(("rep", "grp"), "tp")
    return jax.shard_map(per_device_inner, mesh=mesh, in_specs=in_specs, out_specs=out_specs, check_vma=False)
```

```python
import math

import jax
import jax.numpy as jnp
from jax import lax
from jax.experimental import pallas as pl
from jax.experimental.pallas import tpu as pltpu
from jax.sharding import PartitionSpec as P

HEAD_SIZE = 128
PAGE_TOKENS = 128
META_ROWS = 16
NAMED_ROW = 10
LOW = -1e30
CHUNKS = ((0, 1, 7), (2, 6), (3, 5), (4,))
INTERPRET = False


def split3(x):
    hi = x.astype(jnp.bfloat16)
    rest = x - hi.astype(jnp.float32)
    mid = rest.astype(jnp.bfloat16)
    low = (rest - mid.astype(jnp.float32)).astype(jnp.bfloat16)
    return [part.astype(jnp.float32) for part in (hi, mid, low)]


def prepare(queries, block_table, prefix_len, heads_dev, slots):
    req_rows = queries.shape[0]
    list_length = block_table.shape[1]
    cols = heads_dev * req_rows

    def kernel(q_ref, table_ref, length_ref, out_ref):
        for h in range(heads_dev):
            one = q_ref[:, h * HEAD_SIZE : (h + 1) * HEAD_SIZE].astype(jnp.float32)
            out_ref[0:HEAD_SIZE, h * req_rows : (h + 1) * req_rows] = one.T.astype(jnp.bfloat16)
        table = table_ref[...]
        length = length_ref[...]
        slot = lax.broadcasted_iota(jnp.int32, (req_rows, slots), 1)
        hit = jnp.zeros((req_rows, slots), jnp.float32)
        for j in range(list_length):
            entry = jnp.where(PAGE_TOKENS * j < length, table[:, j : j + 1], -1)
            hit = jnp.where(slot == entry, 1.0, hit)
        named = jnp.max(hit, axis=0, keepdims=True)
        high = lax.div(length, 8)
        small = jnp.concatenate([table, high, length - 8 * high], axis=1).astype(jnp.float32)
        small = jnp.concatenate([small, jnp.zeros((req_rows, HEAD_SIZE - list_length - 2), jnp.float32)], axis=1)
        small = small.T[0:META_ROWS]
        small = jnp.concatenate([small] * heads_dev, axis=1)
        sub = lax.broadcasted_iota(jnp.int32, (META_ROWS, cols), 0)
        out_ref[HEAD_SIZE:] = jnp.where(sub == list_length + 2, named, small).astype(jnp.bfloat16)

    return pl.pallas_call(
        kernel,
        out_shape=jax.ShapeDtypeStruct((HEAD_SIZE + META_ROWS, cols), jnp.bfloat16),
        interpret=INTERPRET,
        name="prepare",
    )(queries, block_table, prefix_len.reshape(-1, 1))


def attend_chunk(place, bufs, queries_t, state, shifts, y_count, group_count, per_batch, first, last):
    n_buf = len(bufs)
    buf_rows = bufs[0].shape[0]
    rows, cols = queries_t[0].shape
    limit = 2 * n_buf
    factor = math.log2(math.e) / math.sqrt(HEAD_SIZE)
    int_rows = group_count + 8 * ((n_buf + 7) // 8)

    def kernel(place_ref, *refs):
        buf_refs = refs[:n_buf]
        q_refs = refs[n_buf : n_buf + group_count]
        rest = list(refs[n_buf + group_count :])
        if not first:
            acc_in, ml_in = rest[:2]
            rest = rest[2:]
        if last:
            out_refs = rest[:group_count]
            rest = rest[group_count:]
        else:
            acc_out, ml_out = rest[:2]
            rest = rest[2:]
        (acc, ml, store, query_all, out_all, ints, numbers, item_row, item_slot, sem_store, sem_query, sem_acc, sem_ml, sem_int, sem_out) = rest
        tp_rank = place_ref[0]
        row = place_ref[1]
        core = lax.rem(tp_rank, 2)

        query_copies = [pltpu.make_async_copy(q_refs[g], query_all.at[g], sem_query.at[g]) for g in range(group_count)]
        store_copies = [
            pltpu.make_async_copy(buf_refs[b], store.at[pl.ds(b * buf_rows, buf_rows)], sem_store.at[b]) for b in range(n_buf)
        ]
        for one in query_copies + store_copies:
            one.start()
        if first:
            acc[...] = jnp.zeros(acc.shape, jnp.float32)
            ml[...] = jnp.where(lax.broadcasted_iota(jnp.int32, ml.shape, 1) == 0, LOW, 0.0)
        else:
            ml_copy = pltpu.make_async_copy(ml_in, ml, sem_ml)
            ml_copy.start()
            for g in range(group_count):
                pltpu.make_async_copy(acc_in.at[g], acc.at[g], sem_acc.at[g]).start()
        for one in query_copies + store_copies:
            one.wait()
        for g in range(group_count):
            ints[g : g + 1] = query_all[g, HEAD_SIZE:].astype(jnp.float32)[NAMED_ROW : NAMED_ROW + 1].astype(jnp.int32)
        for b in range(n_buf):
            pages = store[(b + 1) * buf_rows - META_ROWS : (b + 1) * buf_rows].astype(jnp.float32)
            ints[group_count + b : group_count + b + 1, 0:HEAD_SIZE] = pages[0:1].astype(jnp.int32)
        int_copy = pltpu.make_async_copy(ints, numbers, sem_int)
        int_copy.start()
        int_copy.wait()
        if not first:
            ml_copy.wait()

        entry = lax.broadcasted_iota(jnp.int32, (8, cols), 0).astype(jnp.float32)
        token = lax.broadcasted_iota(jnp.int32, (PAGE_TOKENS, cols), 0).astype(jnp.float32)

        def group(g, _):
            number = lax.rem(row + group_count - g, group_count)
            count = jnp.int32(0)
            for b in range(n_buf):
                source_y = lax.rem(lax.div(tp_rank, 2) + y_count - shifts[b // 2], y_count)
                owner = 2 * source_y + (core if b % 2 == 0 else 1 - core)
                for column in range(2):
                    page = numbers[group_count + b, 2 * number + column]
                    slot = (row * 2 * y_count + owner) * 2 + column
                    used = numbers[g, slot]
                    item_row[count] = b * buf_rows + page * (2 * PAGE_TOKENS)
                    item_slot[count] = slot
                    count = count + jnp.where((page >= 0) & (used > 0), 1, 0)
            for pad in range(per_batch):
                item_row[count + pad] = 0
                item_slot[count + pad] = -1

            table = query_all[g, HEAD_SIZE:].astype(jnp.float32)
            length = table[8:9] * 8.0 + table[9:10]
            table = table[0:8]
            live = jnp.clip(length - PAGE_TOKENS * entry, 0.0, 1.0 * PAGE_TOKENS)
            whole = live == PAGE_TOKENS
            if not first:
                pltpu.make_async_copy(acc_in.at[g], acc.at[g], sem_acc.at[g]).wait()

            def batch(i, _):
                query = query_all[g, 0:HEAD_SIZE]
                starts = [pl.multiple_of(item_row[i * per_batch + j], META_ROWS) for j in range(per_batch)]
                keys = jnp.concatenate([store[pl.ds(start, PAGE_TOKENS)] for start in starts], axis=0)
                raw = jnp.dot(keys, query, preferred_element_type=jnp.float32)
                old = ml[g, 0:1]
                top = old
                scores, counts = [], []
                for j in range(per_batch):
                    slot = item_slot[i * per_batch + j].astype(jnp.float32)
                    match = table == slot
                    full = jnp.sum(jnp.where(match & whole, 1.0, 0.0), axis=0, keepdims=True)
                    part = jnp.max(jnp.where(match & ~whole, live, 0.0), axis=0, keepdims=True)
                    reach = jnp.where(full > 0.0, 1.0 * PAGE_TOKENS, part)
                    score = raw[j * PAGE_TOKENS : (j + 1) * PAGE_TOKENS] * factor
                    score = jnp.where(token < reach, score, LOW)
                    top = jnp.maximum(top, jnp.max(score, axis=0, keepdims=True))
                    scores.append(score)
                    counts.append((full, part))
                shrink = jnp.exp2(old - top)
                total = ml[g, 1:2] * shrink
                weights = []
                for j in range(per_batch):
                    full, part = counts[j]
                    weight = jnp.exp2(scores[j] - top) * jnp.where(token < part, full + 1.0, full)
                    total = total + jnp.sum(weight, axis=0, keepdims=True)
                    weights.append(weight.astype(jnp.bfloat16))
                values = jnp.concatenate([store[pl.ds(start + PAGE_TOKENS, PAGE_TOKENS)] for start in starts], axis=0)
                added = lax.dot_general(
                    values, jnp.concatenate(weights, axis=0), (((0,), (0,)), ((), ())), preferred_element_type=jnp.float32
                )
                acc[g] = acc[g] * shrink + added
                ml[g, 0:1] = top
                ml[g, 1:2] = total
                return 0

            lax.fori_loop(0, lax.div(count + per_batch - 1, per_batch), batch, 0)

            if last:
                top = ml[g, 0:1]
                total = ml[g, 1:2]
                inverse = jnp.where(total > 0.0, 1.0 / jnp.where(total > 0.0, total, 1.0), 0.0)
                out_all[g, 0:HEAD_SIZE] = (acc[g] * inverse).astype(jnp.bfloat16)
                sub = lax.broadcasted_iota(jnp.int32, (META_ROWS, cols), 0)
                packed = jnp.zeros((META_ROWS, cols), jnp.float32)
                for n, part in enumerate(split3(top) + split3(total)):
                    packed = jnp.where(sub == n, part, packed)
                out_all[g, HEAD_SIZE:] = packed.astype(jnp.bfloat16)
                for n in range(group_count):

                    @pl.when(g == n)
                    def _():
                        pltpu.make_async_copy(out_all.at[n], out_refs[n], sem_out.at[n]).start()
            else:
                pltpu.make_async_copy(acc.at[g], acc_out.at[g], sem_out.at[g]).start()
            return 0

        lax.fori_loop(0, group_count, group, 0)
        if last:
            for n in range(group_count):
                pltpu.make_async_copy(out_all.at[n], out_refs[n], sem_out.at[n]).wait()
        else:
            ml_back = pltpu.make_async_copy(ml, ml_out, sem_ml)
            ml_back.start()
            for n in range(group_count):
                pltpu.make_async_copy(acc.at[n], acc_out.at[n], sem_out.at[n]).wait()
            ml_back.wait()

    if last:
        out_shape = [jax.ShapeDtypeStruct((HEAD_SIZE + META_ROWS, cols), jnp.bfloat16)] * group_count
    else:
        out_shape = [
            jax.ShapeDtypeStruct((group_count, HEAD_SIZE, cols), jnp.float32),
            jax.ShapeDtypeStruct((group_count, 8, cols), jnp.float32),
        ]
    n_out_slots = group_count if last else 1
    scratch = [
        pltpu.VMEM((group_count, HEAD_SIZE, cols), jnp.float32),
        pltpu.VMEM((group_count, 8, cols), jnp.float32),
        pltpu.VMEM((n_buf * buf_rows, HEAD_SIZE), jnp.bfloat16),
        pltpu.VMEM((group_count, rows, cols), jnp.bfloat16),
        pltpu.VMEM((n_out_slots, HEAD_SIZE + META_ROWS, cols), jnp.bfloat16),
        pltpu.VMEM((int_rows, cols), jnp.int32),
        pltpu.SMEM((int_rows, cols), jnp.int32),
        pltpu.SMEM((limit + per_batch,), jnp.int32),
        pltpu.SMEM((limit + per_batch,), jnp.int32),
        pltpu.SemaphoreType.DMA((n_buf,)),
        pltpu.SemaphoreType.DMA((group_count,)),
        pltpu.SemaphoreType.DMA((group_count,)),
        pltpu.SemaphoreType.DMA,
        pltpu.SemaphoreType.DMA,
        pltpu.SemaphoreType.DMA((group_count,)),
    ]
    anywhere = pl.BlockSpec(memory_space=pltpu.MemorySpace.HBM)
    n_in = n_buf + group_count + (0 if first else 2)
    return pl.pallas_call(
        kernel,
        out_shape=out_shape,
        grid_spec=pltpu.PrefetchScalarGridSpec(
            num_scalar_prefetch=1,
            grid=(),
            in_specs=[anywhere] * n_in,
            out_specs=[anywhere] * len(out_shape),
            scratch_shapes=scratch,
        ),
        interpret=INTERPRET,
    )(place, *bufs, *queries_t, *(() if first else state))


def combine(arrived, query_t, newest_t, heads_dev):
    parts = len(arrived)
    cols = arrived[0].shape[1]
    req_rows = cols // heads_dev
    factor = math.log2(math.e) / math.sqrt(HEAD_SIZE)

    def kernel(*refs):
        in_refs = refs[:parts]
        q_ref, new_ref, out_ref = refs[parts:]
        query = q_ref[0:HEAD_SIZE].astype(jnp.float32)
        own = jnp.sum(query * new_ref[0].astype(jnp.float32), axis=0, keepdims=True) * factor
        top = own
        tops, totals = [], []
        for n in range(parts):
            packed = in_refs[n][HEAD_SIZE:].astype(jnp.float32)
            tops.append(packed[0:1] + packed[1:2] + packed[2:3])
            totals.append(packed[3:4] + packed[4:5] + packed[5:6])
            top = jnp.maximum(top, tops[-1])
        own_weight = jnp.exp2(own - top)
        denominator = own_weight
        scales = []
        for n in range(parts):
            scales.append(totals[n] * jnp.exp2(tops[n] - top))
            denominator = denominator + scales[-1]
        inverse = 1.0 / denominator
        mix = new_ref[1].astype(jnp.float32) * (own_weight * inverse)
        for n in range(parts):
            mix = mix + in_refs[n][0:HEAD_SIZE].astype(jnp.float32) * (scales[n] * inverse)
        for h in range(heads_dev):
            one = mix[:, h * req_rows : (h + 1) * req_rows]
            out_ref[:, h * HEAD_SIZE : (h + 1) * HEAD_SIZE] = one.T.astype(jnp.bfloat16)

    return pl.pallas_call(
        kernel,
        out_shape=jax.ShapeDtypeStruct((req_rows, heads_dev * HEAD_SIZE), jnp.bfloat16),
        interpret=INTERPRET,
        name="combine",
    )(*arrived, query_t, newest_t)


def project(place, mix_own, mix_partner, weight_own, weight_partner, y_count):
    width = weight_own.shape[1] // (2 * y_count)
    req_rows, depth = mix_own.shape

    def kernel(place_ref, own_ref, partner_ref, w_own_ref, w_partner_ref, out_ref, w_all, sem):
        core = lax.rem(place_ref[0], 2)
        copies = []
        for n in range(y_count):
            start = pl.multiple_of((2 * n + core) * width, width)
            for k, ref in enumerate((w_own_ref, w_partner_ref)):
                copies.append(
                    pltpu.make_async_copy(
                        ref.at[:, pl.ds(start, width)], w_all.at[n, pl.ds(k * depth, depth)], sem.at[2 * n + k]
                    )
                )
        for one in copies:
            one.start()
        mix = jnp.concatenate([own_ref[...], partner_ref[...]], axis=1)
        for n in range(y_count):
            copies[2 * n].wait()
            copies[2 * n + 1].wait()
            out_ref[n] = jnp.dot(mix, w_all[n], preferred_element_type=jnp.float32).astype(jnp.bfloat16)

    vmem = pl.BlockSpec(memory_space=pltpu.MemorySpace.VMEM)
    anywhere = pl.BlockSpec(memory_space=pltpu.MemorySpace.HBM)
    return pl.pallas_call(
        kernel,
        out_shape=jax.ShapeDtypeStruct((y_count, req_rows, width), jnp.bfloat16),
        grid_spec=pltpu.PrefetchScalarGridSpec(
            num_scalar_prefetch=1,
            grid=(),
            in_specs=[vmem, vmem, anywhere, anywhere],
            out_specs=vmem,
            scratch_shapes=[
                pltpu.VMEM((y_count, 2 * depth, width), jnp.bfloat16),
                pltpu.SemaphoreType.DMA((2 * y_count,)),
            ],
        ),
        interpret=INTERPRET,
        name="project",
    )(place, mix_own, mix_partner, weight_own, weight_partner)


def per_device_inner(
    queries, newest_key_value, kv_pages, fetch_slots, block_table, prefix_len, out_weight
):
    tp_count = lax.axis_size("tp")
    group_count = lax.axis_size("grp")
    y_count = tp_count // 2
    tp_rank = lax.axis_index("tp").astype(jnp.int32)
    row = lax.axis_index("grp").astype(jnp.int32)
    y = lax.div(tp_rank, 2)
    heads_dev = queries.shape[1] // HEAD_SIZE
    slots = 2 * tp_count * group_count
    swap = [(i, i ^ 1) for i in range(tp_count)]

    def along_y(x, shift):
        return lax.ppermute(x, "tp", [(i, (i + 2 * shift) % tp_count) for i in range(tp_count)])

    def along_x(x, shift):
        return lax.ppermute(x, "grp", [(i, (i + shift) % group_count) for i in range(group_count)])

    def to_other_core(x):
        return lax.ppermute(x, "tp", swap)

    slots_block = jnp.pad(fetch_slots.reshape(1, -1).astype(jnp.bfloat16), ((0, META_ROWS - 1), (0, HEAD_SIZE - 2 * group_count)))
    own, partner = {}, {}
    for shift in [s for chunk in CHUNKS for s in chunk]:
        head = lax.rem(y + shift, y_count)
        piece = lax.dynamic_slice_in_dim(kv_pages, head * HEAD_SIZE, HEAD_SIZE, 3)
        piece = jnp.concatenate([piece.reshape(-1, HEAD_SIZE), slots_block], axis=0)
        own[shift] = along_y(piece, shift) if shift else piece
    for shift in own:
        partner[shift] = to_other_core(own[shift])
    weight_partner = to_other_core(out_weight)

    query_t = prepare(queries, block_table, prefix_len, heads_dev, slots)
    queries_t = [along_x(query_t, s) if s else query_t for s in range(group_count)]
    place = jnp.stack([tp_rank, row])

    newest = lax.dynamic_slice_in_dim(newest_key_value, y * HEAD_SIZE, HEAD_SIZE, 2)
    newest_t = jnp.tile(jnp.transpose(newest, (1, 2, 0)), (1, 1, heads_dev))

    state = ()
    for n, shifts in enumerate(CHUNKS):
        bufs = [b for s in shifts for b in (own[s], partner[s])]
        last = n == len(CHUNKS) - 1
        state = attend_chunk(
            place, bufs, queries_t, state, shifts, y_count, group_count, 2 if last else 4, n == 0, last
        )
    arrived = [along_x(state[s], -s) if s else state[s] for s in range(group_count)]

    mix_own = combine(arrived, query_t, newest_t, heads_dev)
    mix_partner = to_other_core(mix_own)
    partial = project(place, mix_own, mix_partner, out_weight, weight_partner, y_count)
    same_core = [[2 * i + c for i in range(y_count)] for c in range(2)]
    arrived = lax.all_to_all(partial, "tp", split_axis=0, concat_axis=0, axis_index_groups=same_core, tiled=True)
    return jnp.sum(arrived.astype(jnp.float32), axis=0).astype(jnp.bfloat16)


def solution(mesh):
    in_specs = (
        P(("rep", "grp"), "tp"),
        P(("rep", "grp"), None, None),
        P(("rep", "grp", "tp"), None, None, None),
        P("rep", ("grp", "tp"), None),
        P(("rep", "grp"), None),
        P(("rep", "grp")),
        P("tp", None),
    )
    out_specs = P(("rep", "grp"), "tp")
    return jax.shard_map(per_device_inner, mesh=mesh, in_specs=in_specs, out_specs=out_specs, check_vma=False)
```

```python
import math

import jax
import jax.numpy as jnp
from jax import lax
from jax.experimental import pallas as pl
from jax.experimental.pallas import tpu as pltpu
from jax.sharding import PartitionSpec as P

HEAD_SIZE = 128
PAGE_TOKENS = 128
META_ROWS = 16
NAMED_ROW = 10
LOW = -1e30
CHUNKS = ((0, 1, 7, 2, 6), (3, 5, 4))
STAT_ROWS = 16
INTERPRET = False


def split3(x):
    hi = x.astype(jnp.bfloat16)
    rest = x - hi.astype(jnp.float32)
    mid = rest.astype(jnp.bfloat16)
    low = (rest - mid.astype(jnp.float32)).astype(jnp.bfloat16)
    return [part.astype(jnp.float32) for part in (hi, mid, low)]


def prepare(queries, block_table, prefix_len, heads_dev, slots):
    req_rows = queries.shape[0]
    list_length = block_table.shape[1]
    cols = heads_dev * req_rows
    assert slots == cols

    def kernel(q_ref, table_ref, length_ref, out_ref):
        for h in range(heads_dev):
            one = q_ref[:, h * HEAD_SIZE : (h + 1) * HEAD_SIZE].astype(jnp.float32)
            out_ref[0:HEAD_SIZE, h * req_rows : (h + 1) * req_rows] = one.T.astype(jnp.bfloat16)
        length = length_ref[...]
        high = lax.div(length, 8)
        small = jnp.concatenate([table_ref[...], high, length - 8 * high, length], axis=0).astype(jnp.float32)
        small = jnp.concatenate([small, jnp.zeros((HEAD_SIZE - list_length - 3, req_rows), jnp.float32)], axis=0)
        lists = small.T
        slot = lax.broadcasted_iota(jnp.int32, (req_rows, slots), 1).astype(jnp.float32)
        hit = jnp.zeros((req_rows, slots), jnp.float32)
        for j in range(list_length):
            entry = jnp.where(lists[:, list_length + 2 : list_length + 3] > PAGE_TOKENS * j, lists[:, j : j + 1], -1.0)
            hit = jnp.where(slot == entry, 1.0, hit)
        named = jnp.max(hit, axis=0, keepdims=True)
        small = jnp.concatenate([small[0:META_ROWS]] * heads_dev, axis=1)
        sub = lax.broadcasted_iota(jnp.int32, (META_ROWS, cols), 0)
        out_ref[HEAD_SIZE:] = jnp.where(sub == list_length + 2, named, small).astype(jnp.bfloat16)

    return pl.pallas_call(
        kernel,
        out_shape=jax.ShapeDtypeStruct((HEAD_SIZE + META_ROWS, cols), jnp.bfloat16),
        interpret=INTERPRET,
        name="prepare",
    )(queries, block_table.T, prefix_len.reshape(1, -1))


def attend_chunk(place, bufs, queries_t, state, shifts, y_count, group_count, per_batch, first, last):
    n_buf = len(bufs)
    buf_rows = bufs[0].shape[0]
    rows, cols = queries_t[0].shape
    limit = 2 * n_buf
    factor = math.log2(math.e) / math.sqrt(HEAD_SIZE)
    int_rows = group_count + 8 * ((n_buf + 7) // 8)

    def kernel(place_ref, *refs):
        buf_refs = refs[:n_buf]
        q_refs = refs[n_buf : n_buf + group_count]
        rest = list(refs[n_buf + group_count :])
        if not first:
            acc_in, ml_in = rest[:2]
            rest = rest[2:]
        if last:
            out_ref = rest[0]
            rest = rest[1:]
        else:
            acc_out, ml_out = rest[:2]
            rest = rest[2:]
        (acc, ml, store, query_all, out_all, ints, numbers, item_row, item_slot, sem_store, sem_query, sem_acc, sem_ml, sem_int, sem_out) = rest
        tp_rank = place_ref[0]
        row = place_ref[1]
        core = lax.rem(tp_rank, 2)

        query_copies = [pltpu.make_async_copy(q_refs[g], query_all.at[g], sem_query.at[g]) for g in range(group_count)]
        store_copies = [
            pltpu.make_async_copy(buf_refs[b], store.at[pl.ds(b * buf_rows, buf_rows)], sem_store.at[b]) for b in range(n_buf)
        ]
        for one in query_copies + store_copies:
            one.start()
        if first:
            acc[...] = jnp.zeros(acc.shape, jnp.float32)
            ml[...] = jnp.where(lax.broadcasted_iota(jnp.int32, ml.shape, 1) == 0, LOW, 0.0)
        else:
            ml_copy = pltpu.make_async_copy(ml_in, ml, sem_ml)
            ml_copy.start()
            for g in range(group_count):
                pltpu.make_async_copy(acc_in.at[g], acc.at[g], sem_acc.at[g]).start()
        for one in query_copies + store_copies:
            one.wait()
        for g in range(group_count):
            ints[g : g + 1] = query_all[g, HEAD_SIZE:].astype(jnp.float32)[NAMED_ROW : NAMED_ROW + 1].astype(jnp.int32)
        for b in range(n_buf):
            pages = store[(b + 1) * buf_rows - META_ROWS : (b + 1) * buf_rows].astype(jnp.float32)
            ints[group_count + b : group_count + b + 1, 0:HEAD_SIZE] = pages[0:1].astype(jnp.int32)
        int_copy = pltpu.make_async_copy(ints, numbers, sem_int)
        int_copy.start()
        int_copy.wait()
        if not first:
            ml_copy.wait()

        entry = lax.broadcasted_iota(jnp.int32, (8, cols), 0).astype(jnp.float32)
        token = lax.broadcasted_iota(jnp.int32, (PAGE_TOKENS, cols), 0).astype(jnp.float32)

        def group(g, _):
            number = lax.rem(row + group_count - g, group_count)
            count = jnp.int32(0)
            for b in range(n_buf):
                source_y = lax.rem(lax.div(tp_rank, 2) + y_count - shifts[b // 2], y_count)
                owner = 2 * source_y + (core if b % 2 == 0 else 1 - core)
                for column in range(2):
                    page = numbers[group_count + b, 2 * number + column]
                    slot = (row * 2 * y_count + owner) * 2 + column
                    used = numbers[g, slot]
                    item_row[count] = b * buf_rows + page * (2 * PAGE_TOKENS)
                    item_slot[count] = slot
                    count = count + jnp.where((page >= 0) & (used > 0), 1, 0)
            for pad in range(per_batch):
                item_row[count + pad] = 0
                item_slot[count + pad] = -1

            table = query_all[g, HEAD_SIZE:].astype(jnp.float32)
            length = table[8:9] * 8.0 + table[9:10]
            table = table[0:8]
            live = jnp.clip(length - PAGE_TOKENS * entry, 0.0, 1.0 * PAGE_TOKENS)
            whole = live == PAGE_TOKENS
            if not first:
                pltpu.make_async_copy(acc_in.at[g], acc.at[g], sem_acc.at[g]).wait()

            def batch(i, _):
                query = query_all[g, 0:HEAD_SIZE]
                starts = [pl.multiple_of(item_row[i * per_batch + j], META_ROWS) for j in range(per_batch)]
                keys = jnp.concatenate([store[pl.ds(start, PAGE_TOKENS)] for start in starts], axis=0)
                raw = jnp.dot(keys, query, preferred_element_type=jnp.float32)
                old = ml[g, 0:1]
                top = old
                scores, counts = [], []
                for j in range(per_batch):
                    slot = item_slot[i * per_batch + j].astype(jnp.float32)
                    match = table == slot
                    full = jnp.sum(jnp.where(match & whole, 1.0, 0.0), axis=0, keepdims=True)
                    part = jnp.max(jnp.where(match & ~whole, live, 0.0), axis=0, keepdims=True)
                    reach = jnp.where(full > 0.0, 1.0 * PAGE_TOKENS, part)
                    score = raw[j * PAGE_TOKENS : (j + 1) * PAGE_TOKENS] * factor
                    score = jnp.where(token < reach, score, LOW)
                    top = jnp.maximum(top, jnp.max(score, axis=0, keepdims=True))
                    scores.append(score)
                    counts.append((full, part))
                shrink = jnp.exp2(old - top)
                total = ml[g, 1:2] * shrink
                weights = []
                for j in range(per_batch):
                    full, part = counts[j]
                    weight = jnp.exp2(scores[j] - top) * jnp.where(token < part, full + 1.0, full)
                    total = total + jnp.sum(weight, axis=0, keepdims=True)
                    weights.append(weight.astype(jnp.bfloat16))
                values = jnp.concatenate([store[pl.ds(start + PAGE_TOKENS, PAGE_TOKENS)] for start in starts], axis=0)
                added = lax.dot_general(
                    values, jnp.concatenate(weights, axis=0), (((0,), (0,)), ((), ())), preferred_element_type=jnp.float32
                )
                acc[g] = acc[g] * shrink + added
                ml[g, 0:1] = top
                ml[g, 1:2] = total
                return 0

            lax.fori_loop(0, lax.div(count + per_batch - 1, per_batch), batch, 0)

            if last:
                top = ml[g, 0:1]
                total = ml[g, 1:2]
                inverse = jnp.where(total > 0.0, 1.0 / jnp.where(total > 0.0, total, 1.0), 0.0)
                out_all[g, 0:HEAD_SIZE] = (acc[g] * inverse).astype(jnp.bfloat16)
                sub = lax.broadcasted_iota(jnp.int32, (STAT_ROWS, cols), 0)
                packed = jnp.zeros((STAT_ROWS, cols), jnp.float32)
                for n, part in enumerate(split3(top) + split3(total)):
                    packed = jnp.where(sub == n, part, packed)
                out_all[g, HEAD_SIZE:] = packed.astype(jnp.bfloat16)
                pltpu.make_async_copy(out_all.at[g], out_ref.at[number], sem_out.at[g]).start()
            else:
                pltpu.make_async_copy(acc.at[g], acc_out.at[g], sem_out.at[g]).start()
            return 0

        lax.fori_loop(0, group_count, group, 0)
        if last:
            for n in range(group_count):
                pltpu.make_async_copy(out_all.at[n], out_ref.at[n], sem_out.at[n]).wait()
        else:
            ml_back = pltpu.make_async_copy(ml, ml_out, sem_ml)
            ml_back.start()
            for n in range(group_count):
                pltpu.make_async_copy(acc.at[n], acc_out.at[n], sem_out.at[n]).wait()
            ml_back.wait()

    if last:
        out_shape = [jax.ShapeDtypeStruct((group_count, HEAD_SIZE + STAT_ROWS, cols), jnp.bfloat16)]
    else:
        out_shape = [
            jax.ShapeDtypeStruct((group_count, HEAD_SIZE, cols), jnp.float32),
            jax.ShapeDtypeStruct((group_count, 8, cols), jnp.float32),
        ]
    n_out_slots = group_count if last else 1
    scratch = [
        pltpu.VMEM((group_count, HEAD_SIZE, cols), jnp.float32),
        pltpu.VMEM((group_count, 8, cols), jnp.float32),
        pltpu.VMEM((n_buf * buf_rows, HEAD_SIZE), jnp.bfloat16),
        pltpu.VMEM((group_count, rows, cols), jnp.bfloat16),
        pltpu.VMEM((n_out_slots, HEAD_SIZE + STAT_ROWS, cols), jnp.bfloat16),
        pltpu.VMEM((int_rows, cols), jnp.int32),
        pltpu.SMEM((int_rows, cols), jnp.int32),
        pltpu.SMEM((limit + per_batch,), jnp.int32),
        pltpu.SMEM((limit + per_batch,), jnp.int32),
        pltpu.SemaphoreType.DMA((n_buf,)),
        pltpu.SemaphoreType.DMA((group_count,)),
        pltpu.SemaphoreType.DMA((group_count,)),
        pltpu.SemaphoreType.DMA,
        pltpu.SemaphoreType.DMA,
        pltpu.SemaphoreType.DMA((group_count,)),
    ]
    anywhere = pl.BlockSpec(memory_space=pltpu.MemorySpace.HBM)
    n_in = n_buf + group_count + (0 if first else 2)
    return pl.pallas_call(
        kernel,
        out_shape=out_shape,
        grid_spec=pltpu.PrefetchScalarGridSpec(
            num_scalar_prefetch=1,
            grid=(),
            in_specs=[anywhere] * n_in,
            out_specs=[anywhere] * len(out_shape),
            scratch_shapes=scratch,
        ),
        interpret=INTERPRET,
    )(place, *bufs, *queries_t, *(() if first else state))


def combine(arrived, query_t, newest_t, heads_dev):
    parts, _, cols = arrived.shape
    req_rows = cols // heads_dev
    factor = math.log2(math.e) / math.sqrt(HEAD_SIZE)

    def kernel(in_ref, q_ref, new_ref, out_ref):
        query = q_ref[0:HEAD_SIZE].astype(jnp.float32)
        own = jnp.sum(query * new_ref[0].astype(jnp.float32), axis=0, keepdims=True) * factor
        top = own
        tops, totals = [], []
        for n in range(parts):
            packed = in_ref[n, HEAD_SIZE:].astype(jnp.float32)
            tops.append(packed[0:1] + packed[1:2] + packed[2:3])
            totals.append(packed[3:4] + packed[4:5] + packed[5:6])
            top = jnp.maximum(top, tops[-1])
        own_weight = jnp.exp2(own - top)
        denominator = own_weight
        scales = []
        for n in range(parts):
            scales.append(totals[n] * jnp.exp2(tops[n] - top))
            denominator = denominator + scales[-1]
        inverse = 1.0 / denominator
        mix = new_ref[1].astype(jnp.float32) * (own_weight * inverse)
        for n in range(parts):
            mix = mix + in_ref[n, 0:HEAD_SIZE].astype(jnp.float32) * (scales[n] * inverse)
        for h in range(heads_dev):
            one = mix[:, h * req_rows : (h + 1) * req_rows]
            out_ref[:, h * HEAD_SIZE : (h + 1) * HEAD_SIZE] = one.T.astype(jnp.bfloat16)

    return pl.pallas_call(
        kernel,
        out_shape=jax.ShapeDtypeStruct((req_rows, heads_dev * HEAD_SIZE), jnp.bfloat16),
        interpret=INTERPRET,
        name="combine",
    )(arrived, query_t, newest_t)


def project(place, mix_own, mix_partner, weight_own, weight_partner, y_count):
    width = weight_own.shape[1] // (2 * y_count)
    req_rows, depth = mix_own.shape

    def kernel(place_ref, own_ref, partner_ref, w_own_ref, w_partner_ref, out_ref, w_all, sem):
        core = lax.rem(place_ref[0], 2)
        copies = []
        for n in range(y_count):
            start = pl.multiple_of((2 * n + core) * width, width)
            for k, ref in enumerate((w_own_ref, w_partner_ref)):
                copies.append(
                    pltpu.make_async_copy(
                        ref.at[:, pl.ds(start, width)], w_all.at[n, pl.ds(k * depth, depth)], sem.at[2 * n + k]
                    )
                )
        for one in copies:
            one.start()
        mix = jnp.concatenate([own_ref[...], partner_ref[...]], axis=1)
        for n in range(y_count):
            copies[2 * n].wait()
            copies[2 * n + 1].wait()
            out_ref[n] = jnp.dot(mix, w_all[n], preferred_element_type=jnp.float32).astype(jnp.bfloat16)

    vmem = pl.BlockSpec(memory_space=pltpu.MemorySpace.VMEM)
    anywhere = pl.BlockSpec(memory_space=pltpu.MemorySpace.HBM)
    return pl.pallas_call(
        kernel,
        out_shape=jax.ShapeDtypeStruct((y_count, req_rows, width), jnp.bfloat16),
        grid_spec=pltpu.PrefetchScalarGridSpec(
            num_scalar_prefetch=1,
            grid=(),
            in_specs=[vmem, vmem, anywhere, anywhere],
            out_specs=vmem,
            scratch_shapes=[
                pltpu.VMEM((y_count, 2 * depth, width), jnp.bfloat16),
                pltpu.SemaphoreType.DMA((2 * y_count,)),
            ],
        ),
        interpret=INTERPRET,
        name="project",
    )(place, mix_own, mix_partner, weight_own, weight_partner)


def per_device_inner(
    queries, newest_key_value, kv_pages, fetch_slots, block_table, prefix_len, out_weight
):
    tp_count = lax.axis_size("tp")
    group_count = lax.axis_size("grp")
    y_count = tp_count // 2
    tp_rank = lax.axis_index("tp").astype(jnp.int32)
    row = lax.axis_index("grp").astype(jnp.int32)
    y = lax.div(tp_rank, 2)
    heads_dev = queries.shape[1] // HEAD_SIZE
    slots = 2 * tp_count * group_count
    swap = [(i, i ^ 1) for i in range(tp_count)]

    def along_y(x, shift):
        return lax.ppermute(x, "tp", [(i, (i + 2 * shift) % tp_count) for i in range(tp_count)])

    def along_x(x, shift):
        return lax.ppermute(x, "grp", [(i, (i + shift) % group_count) for i in range(group_count)])

    def to_other_core(x):
        return lax.ppermute(x, "tp", swap)

    slots_block = jnp.pad(fetch_slots.reshape(1, -1).astype(jnp.bfloat16), ((0, META_ROWS - 1), (0, HEAD_SIZE - 2 * group_count)))
    own, partner = {}, {}
    for shift in [s for chunk in CHUNKS for s in chunk]:
        head = lax.rem(y + shift, y_count)
        piece = lax.dynamic_slice_in_dim(kv_pages, head * HEAD_SIZE, HEAD_SIZE, 3)
        piece = jnp.concatenate([piece.reshape(-1, HEAD_SIZE), slots_block], axis=0)
        own[shift] = along_y(piece, shift) if shift else piece
    for shift in own:
        partner[shift] = to_other_core(own[shift])
    weight_partner = to_other_core(out_weight)

    query_t = prepare(queries, block_table, prefix_len, heads_dev, slots)
    queries_t = [along_x(query_t, s) if s else query_t for s in range(group_count)]
    place = jnp.stack([tp_rank, row])

    newest = lax.dynamic_slice_in_dim(newest_key_value, y * HEAD_SIZE, HEAD_SIZE, 2)
    newest_t = jnp.tile(jnp.transpose(newest, (1, 2, 0)), (1, 1, heads_dev))

    state = ()
    for n, shifts in enumerate(CHUNKS):
        bufs = [b for s in shifts for b in (own[s], partner[s])]
        last = n == len(CHUNKS) - 1
        state = attend_chunk(
            place, bufs, queries_t, state, shifts, y_count, group_count, 4, n == 0, last
        )
    arrived = lax.all_to_all(state[0], "grp", split_axis=0, concat_axis=0, tiled=True)

    mix_own = combine(arrived, query_t, newest_t, heads_dev)
    mix_partner = to_other_core(mix_own)
    partial = project(place, mix_own, mix_partner, out_weight, weight_partner, y_count)
    same_core = [[2 * i + c for i in range(y_count)] for c in range(2)]
    arrived = lax.all_to_all(partial, "tp", split_axis=0, concat_axis=0, axis_index_groups=same_core, tiled=True)
    return jnp.sum(arrived.astype(jnp.float32), axis=0).astype(jnp.bfloat16)


def solution(mesh):
    in_specs = (
        P(("rep", "grp"), "tp"),
        P(("rep", "grp"), None, None),
        P(("rep", "grp", "tp"), None, None, None),
        P("rep", ("grp", "tp"), None),
        P(("rep", "grp"), None),
        P(("rep", "grp")),
        P("tp", None),
    )
    out_specs = P(("rep", "grp"), "tp")
    return jax.shard_map(per_device_inner, mesh=mesh, in_specs=in_specs, out_specs=out_specs, check_vma=False)
```

```python
import math

import jax
import jax.numpy as jnp
from jax import lax
from jax.experimental import pallas as pl
from jax.experimental.pallas import tpu as pltpu
from jax.sharding import PartitionSpec as P

HEAD_SIZE = 128
PAGE_TOKENS = 128
META_ROWS = 16
NAMED_ROW = 10
LOW = -1e30
CHUNKS = ((0, 1, 7, 2, 6), (3, 5, 4))
STAT_ROWS = 16
INTERPRET = False


def split3(x):
    hi = x.astype(jnp.bfloat16)
    rest = x - hi.astype(jnp.float32)
    mid = rest.astype(jnp.bfloat16)
    low = (rest - mid.astype(jnp.float32)).astype(jnp.bfloat16)
    return [part.astype(jnp.float32) for part in (hi, mid, low)]


def prepare(queries, block_table, prefix_len, heads_dev, slots, group_count):
    req_rows = queries.shape[0]
    list_length = block_table.shape[1]
    cols = heads_dev * req_rows
    assert slots == cols

    def kernel(q_ref, table_ref, length_ref, out_ref):
        heads = [q_ref[:, h * HEAD_SIZE : (h + 1) * HEAD_SIZE].astype(jnp.float32).T for h in range(heads_dev)]
        query = jnp.concatenate(heads, axis=1).astype(jnp.bfloat16)
        length = length_ref[...]
        high = lax.div(length, 8)
        small = jnp.concatenate([table_ref[...], high, length - 8 * high, length], axis=0).astype(jnp.float32)
        small = jnp.concatenate([small, jnp.zeros((HEAD_SIZE - list_length - 3, req_rows), jnp.float32)], axis=0)
        lists = small.T
        slot = lax.broadcasted_iota(jnp.int32, (req_rows, slots), 1).astype(jnp.float32)
        hit = jnp.zeros((req_rows, slots), jnp.float32)
        for j in range(list_length):
            entry = jnp.where(lists[:, list_length + 2 : list_length + 3] > PAGE_TOKENS * j, lists[:, j : j + 1], -1.0)
            hit = jnp.where(slot == entry, 1.0, hit)
        named = jnp.max(hit, axis=0, keepdims=True)
        small = jnp.concatenate([small[0:META_ROWS]] * heads_dev, axis=1)
        sub = lax.broadcasted_iota(jnp.int32, (META_ROWS, cols), 0)
        small = jnp.where(sub == list_length + 2, named, small).astype(jnp.bfloat16)
        for g in range(group_count):
            out_ref[g, 0:HEAD_SIZE] = query
            out_ref[g, HEAD_SIZE:] = small

    return pl.pallas_call(
        kernel,
        out_shape=jax.ShapeDtypeStruct((group_count, HEAD_SIZE + META_ROWS, cols), jnp.bfloat16),
        interpret=INTERPRET,
        name="prepare",
    )(queries, block_table.T, prefix_len.reshape(1, -1))


def attend_chunk(place, bufs, queries_t, state, shifts, y_count, per_batch, first, last):
    n_buf = len(bufs)
    buf_rows = bufs[0].shape[0]
    group_count, rows, cols = queries_t.shape
    limit = 2 * n_buf
    factor = math.log2(math.e) / math.sqrt(HEAD_SIZE)
    int_rows = group_count + 8 * ((n_buf + 7) // 8)

    def kernel(place_ref, *refs):
        buf_refs = refs[:n_buf]
        q_ref = refs[n_buf]
        rest = list(refs[n_buf + 1 :])
        if not first:
            acc_in, ml_in = rest[:2]
            rest = rest[2:]
        if last:
            out_ref = rest[0]
            rest = rest[1:]
        else:
            acc_out, ml_out = rest[:2]
            rest = rest[2:]
        (acc, ml, store, lists, query_all, out_all, ints, numbers, item_row, item_slot, sem_store, sem_list, sem_query, sem_acc, sem_ml, sem_int, sem_out) = rest
        tp_rank = place_ref[0]
        row = place_ref[1]
        core = lax.rem(tp_rank, 2)

        query_copies = [pltpu.make_async_copy(q_ref.at[g], query_all.at[g], sem_query.at[g]) for g in range(group_count)]
        store_copies = [
            pltpu.make_async_copy(buf_refs[b], store.at[pl.ds(b * buf_rows, buf_rows)], sem_store.at[b]) for b in range(n_buf)
        ]
        list_copies = [
            pltpu.make_async_copy(buf_refs[b].at[pl.ds(buf_rows - META_ROWS, META_ROWS)], lists.at[b], sem_list.at[b])
            for b in range(n_buf)
        ]
        for one in list_copies + query_copies + store_copies:
            one.start()
        if first:
            acc[...] = jnp.zeros(acc.shape, jnp.float32)
            ml[...] = jnp.where(lax.broadcasted_iota(jnp.int32, ml.shape, 1) == 0, LOW, 0.0)
        else:
            ml_copy = pltpu.make_async_copy(ml_in, ml, sem_ml)
            ml_copy.start()
            for g in range(group_count):
                pltpu.make_async_copy(acc_in.at[g], acc.at[g], sem_acc.at[g]).start()
        for one in list_copies + query_copies:
            one.wait()
        for g in range(group_count):
            ints[g : g + 1] = query_all[g, HEAD_SIZE:].astype(jnp.float32)[NAMED_ROW : NAMED_ROW + 1].astype(jnp.int32)
        for b in range(n_buf):
            pages = lists[b].astype(jnp.float32)
            ints[group_count + b : group_count + b + 1, 0:HEAD_SIZE] = pages[0:1].astype(jnp.int32)
        int_copy = pltpu.make_async_copy(ints, numbers, sem_int)
        int_copy.start()
        int_copy.wait()
        if not first:
            ml_copy.wait()
        for one in store_copies:
            one.wait()

        entry = lax.broadcasted_iota(jnp.int32, (8, cols), 0).astype(jnp.float32)
        token = lax.broadcasted_iota(jnp.int32, (PAGE_TOKENS, cols), 0).astype(jnp.float32)

        def group(g, _):
            count = jnp.int32(0)
            for b in range(n_buf):
                source_y = lax.rem(lax.div(tp_rank, 2) + y_count - shifts[b // 2], y_count)
                owner = 2 * source_y + (core if b % 2 == 0 else 1 - core)
                for column in range(2):
                    page = numbers[group_count + b, 2 * g + column]
                    slot = (row * 2 * y_count + owner) * 2 + column
                    used = numbers[g, slot]
                    item_row[count] = b * buf_rows + page * (2 * PAGE_TOKENS)
                    item_slot[count] = slot
                    count = count + jnp.where((page >= 0) & (used > 0), 1, 0)
            for pad in range(per_batch):
                item_row[count + pad] = 0
                item_slot[count + pad] = -1

            table = query_all[g, HEAD_SIZE:].astype(jnp.float32)
            length = table[8:9] * 8.0 + table[9:10]
            table = table[0:8]
            live = jnp.clip(length - PAGE_TOKENS * entry, 0.0, 1.0 * PAGE_TOKENS)
            whole = live == PAGE_TOKENS
            if not first:
                pltpu.make_async_copy(acc_in.at[g], acc.at[g], sem_acc.at[g]).wait()

            def batch(i, _):
                query = query_all[g, 0:HEAD_SIZE]
                starts = [pl.multiple_of(item_row[i * per_batch + j], META_ROWS) for j in range(per_batch)]
                keys = jnp.concatenate([store[pl.ds(start, PAGE_TOKENS)] for start in starts], axis=0)
                raw = jnp.dot(keys, query, preferred_element_type=jnp.float32)
                old = ml[g, 0:1]
                top = old
                scores, counts = [], []
                for j in range(per_batch):
                    slot = item_slot[i * per_batch + j].astype(jnp.float32)
                    match = table == slot
                    full = jnp.sum(jnp.where(match & whole, 1.0, 0.0), axis=0, keepdims=True)
                    part = jnp.max(jnp.where(match & ~whole, live, 0.0), axis=0, keepdims=True)
                    reach = jnp.where(full > 0.0, 1.0 * PAGE_TOKENS, part)
                    score = raw[j * PAGE_TOKENS : (j + 1) * PAGE_TOKENS] * factor
                    score = jnp.where(token < reach, score, LOW)
                    top = jnp.maximum(top, jnp.max(score, axis=0, keepdims=True))
                    scores.append(score)
                    counts.append((full, part))
                shrink = jnp.exp2(old - top)
                total = ml[g, 1:2] * shrink
                weights = []
                for j in range(per_batch):
                    full, part = counts[j]
                    weight = jnp.exp2(scores[j] - top) * jnp.where(token < part, full + 1.0, full)
                    total = total + jnp.sum(weight, axis=0, keepdims=True)
                    weights.append(weight.astype(jnp.bfloat16))
                values = jnp.concatenate([store[pl.ds(start + PAGE_TOKENS, PAGE_TOKENS)] for start in starts], axis=0)
                added = lax.dot_general(
                    values, jnp.concatenate(weights, axis=0), (((0,), (0,)), ((), ())), preferred_element_type=jnp.float32
                )
                acc[g] = acc[g] * shrink + added
                ml[g, 0:1] = top
                ml[g, 1:2] = total
                return 0

            lax.fori_loop(0, lax.div(count + per_batch - 1, per_batch), batch, 0)

            if last:
                top = ml[g, 0:1]
                total = ml[g, 1:2]
                inverse = jnp.where(total > 0.0, 1.0 / jnp.where(total > 0.0, total, 1.0), 0.0)
                out_all[g, 0:HEAD_SIZE] = (acc[g] * inverse).astype(jnp.bfloat16)
                sub = lax.broadcasted_iota(jnp.int32, (STAT_ROWS, cols), 0)
                packed = jnp.zeros((STAT_ROWS, cols), jnp.float32)
                for n, part in enumerate(split3(top) + split3(total)):
                    packed = jnp.where(sub == n, part, packed)
                out_all[g, HEAD_SIZE:] = packed.astype(jnp.bfloat16)
                pltpu.make_async_copy(out_all.at[g], out_ref.at[g], sem_out.at[g]).start()
            else:
                pltpu.make_async_copy(acc.at[g], acc_out.at[g], sem_out.at[g]).start()
            return 0

        lax.fori_loop(0, group_count, group, 0)
        if last:
            for n in range(group_count):
                pltpu.make_async_copy(out_all.at[n], out_ref.at[n], sem_out.at[n]).wait()
        else:
            ml_back = pltpu.make_async_copy(ml, ml_out, sem_ml)
            ml_back.start()
            for n in range(group_count):
                pltpu.make_async_copy(acc.at[n], acc_out.at[n], sem_out.at[n]).wait()
            ml_back.wait()

    if last:
        out_shape = [jax.ShapeDtypeStruct((group_count, HEAD_SIZE + STAT_ROWS, cols), jnp.bfloat16)]
    else:
        out_shape = [
            jax.ShapeDtypeStruct((group_count, HEAD_SIZE, cols), jnp.float32),
            jax.ShapeDtypeStruct((group_count, 8, cols), jnp.float32),
        ]
    n_out_slots = group_count if last else 1
    scratch = [
        pltpu.VMEM((group_count, HEAD_SIZE, cols), jnp.float32),
        pltpu.VMEM((group_count, 8, cols), jnp.float32),
        pltpu.VMEM((n_buf * buf_rows, HEAD_SIZE), jnp.bfloat16),
        pltpu.VMEM((n_buf, META_ROWS, HEAD_SIZE), jnp.bfloat16),
        pltpu.VMEM((group_count, rows, cols), jnp.bfloat16),
        pltpu.VMEM((n_out_slots, HEAD_SIZE + STAT_ROWS, cols), jnp.bfloat16),
        pltpu.VMEM((int_rows, cols), jnp.int32),
        pltpu.SMEM((int_rows, cols), jnp.int32),
        pltpu.SMEM((limit + per_batch,), jnp.int32),
        pltpu.SMEM((limit + per_batch,), jnp.int32),
        pltpu.SemaphoreType.DMA((n_buf,)),
        pltpu.SemaphoreType.DMA((n_buf,)),
        pltpu.SemaphoreType.DMA((group_count,)),
        pltpu.SemaphoreType.DMA((group_count,)),
        pltpu.SemaphoreType.DMA,
        pltpu.SemaphoreType.DMA,
        pltpu.SemaphoreType.DMA((group_count,)),
    ]
    anywhere = pl.BlockSpec(memory_space=pltpu.MemorySpace.HBM)
    n_in = n_buf + (1 if first else 3)
    return pl.pallas_call(
        kernel,
        out_shape=out_shape,
        grid_spec=pltpu.PrefetchScalarGridSpec(
            num_scalar_prefetch=1,
            grid=(),
            in_specs=[anywhere] * n_in,
            out_specs=[anywhere] * len(out_shape),
            scratch_shapes=scratch,
        ),
        interpret=INTERPRET,
    )(place, *bufs, queries_t, *(() if first else state))


def combine(arrived, query_blocks, newest_t, heads_dev):
    parts, _, cols = arrived.shape
    req_rows = cols // heads_dev
    factor = math.log2(math.e) / math.sqrt(HEAD_SIZE)

    def kernel(in_ref, q_ref, new_ref, out_ref):
        query = q_ref[0, 0:HEAD_SIZE].astype(jnp.float32)
        own = jnp.sum(query * new_ref[0].astype(jnp.float32), axis=0, keepdims=True) * factor
        top = own
        tops, totals = [], []
        for n in range(parts):
            packed = in_ref[n, HEAD_SIZE:].astype(jnp.float32)
            tops.append(packed[0:1] + packed[1:2] + packed[2:3])
            totals.append(packed[3:4] + packed[4:5] + packed[5:6])
            top = jnp.maximum(top, tops[-1])
        own_weight = jnp.exp2(own - top)
        denominator = own_weight
        scales = []
        for n in range(parts):
            scales.append(totals[n] * jnp.exp2(tops[n] - top))
            denominator = denominator + scales[-1]
        inverse = 1.0 / denominator
        mix = new_ref[1].astype(jnp.float32) * (own_weight * inverse)
        for n in range(parts):
            mix = mix + in_ref[n, 0:HEAD_SIZE].astype(jnp.float32) * (scales[n] * inverse)
        for h in range(heads_dev):
            one = mix[:, h * req_rows : (h + 1) * req_rows]
            out_ref[:, h * HEAD_SIZE : (h + 1) * HEAD_SIZE] = one.T.astype(jnp.bfloat16)

    return pl.pallas_call(
        kernel,
        grid=(1,),
        out_shape=jax.ShapeDtypeStruct((req_rows, heads_dev * HEAD_SIZE), jnp.bfloat16),
        in_specs=[
            pl.BlockSpec(arrived.shape, lambda i: (0, 0, 0)),
            pl.BlockSpec((1,) + query_blocks.shape[1:], lambda i: (0, 0, 0)),
            pl.BlockSpec(newest_t.shape, lambda i: (0, 0, 0)),
        ],
        out_specs=pl.BlockSpec((req_rows, heads_dev * HEAD_SIZE), lambda i: (0, 0)),
        interpret=INTERPRET,
        name="combine",
    )(arrived, query_blocks, newest_t)


def project(place, mix_own, mix_partner, weight_own, weight_partner, y_count):
    width = weight_own.shape[1] // (2 * y_count)
    req_rows, depth = mix_own.shape

    def kernel(place_ref, own_ref, partner_ref, w_own_ref, w_partner_ref, out_ref, w_all, sem):
        core = lax.rem(place_ref[0], 2)
        copies = []
        for n in range(y_count):
            start = pl.multiple_of((2 * n + core) * width, width)
            for k, ref in enumerate((w_own_ref, w_partner_ref)):
                copies.append(
                    pltpu.make_async_copy(
                        ref.at[:, pl.ds(start, width)], w_all.at[n, pl.ds(k * depth, depth)], sem.at[2 * n + k]
                    )
                )
        for one in copies:
            one.start()
        mix = jnp.concatenate([own_ref[...], partner_ref[...]], axis=1)
        for n in range(y_count):
            copies[2 * n].wait()
            copies[2 * n + 1].wait()
            out_ref[n] = jnp.dot(mix, w_all[n], preferred_element_type=jnp.float32).astype(jnp.bfloat16)

    vmem = pl.BlockSpec(memory_space=pltpu.MemorySpace.VMEM)
    anywhere = pl.BlockSpec(memory_space=pltpu.MemorySpace.HBM)
    return pl.pallas_call(
        kernel,
        out_shape=jax.ShapeDtypeStruct((y_count, req_rows, width), jnp.bfloat16),
        grid_spec=pltpu.PrefetchScalarGridSpec(
            num_scalar_prefetch=1,
            grid=(),
            in_specs=[vmem, vmem, anywhere, anywhere],
            out_specs=vmem,
            scratch_shapes=[
                pltpu.VMEM((y_count, 2 * depth, width), jnp.bfloat16),
                pltpu.SemaphoreType.DMA((2 * y_count,)),
            ],
        ),
        interpret=INTERPRET,
        name="project",
    )(place, mix_own, mix_partner, weight_own, weight_partner)


def per_device_inner(
    queries, newest_key_value, kv_pages, fetch_slots, block_table, prefix_len, out_weight
):
    tp_count = lax.axis_size("tp")
    group_count = lax.axis_size("grp")
    y_count = tp_count // 2
    tp_rank = lax.axis_index("tp").astype(jnp.int32)
    row = lax.axis_index("grp").astype(jnp.int32)
    y = lax.div(tp_rank, 2)
    heads_dev = queries.shape[1] // HEAD_SIZE
    slots = 2 * tp_count * group_count
    swap = [(i, i ^ 1) for i in range(tp_count)]

    def along_y(x, shift):
        return lax.ppermute(x, "tp", [(i, (i + 2 * shift) % tp_count) for i in range(tp_count)])

    def along_x(x):
        return lax.all_to_all(x, "grp", split_axis=0, concat_axis=0, tiled=True)

    def to_other_core(x):
        return lax.ppermute(x, "tp", swap)

    slots_block = jnp.pad(fetch_slots.reshape(1, -1).astype(jnp.bfloat16), ((0, META_ROWS - 1), (0, HEAD_SIZE - 2 * group_count)))
    own, partner = {}, {}
    for shift in [s for chunk in CHUNKS for s in chunk]:
        head = lax.rem(y + shift, y_count)
        piece = lax.dynamic_slice_in_dim(kv_pages, head * HEAD_SIZE, HEAD_SIZE, 3)
        piece = jnp.concatenate([piece.reshape(-1, HEAD_SIZE), slots_block], axis=0)
        own[shift] = along_y(piece, shift) if shift else piece
    for shift in own:
        partner[shift] = to_other_core(own[shift])
    weight_partner = to_other_core(out_weight)

    query_blocks = prepare(queries, block_table, prefix_len, heads_dev, slots, group_count)
    queries_t = along_x(query_blocks)
    place = jnp.stack([tp_rank, row])

    newest = lax.dynamic_slice_in_dim(newest_key_value, y * HEAD_SIZE, HEAD_SIZE, 2)
    newest_t = jnp.tile(jnp.transpose(newest, (1, 2, 0)), (1, 1, heads_dev))

    state = ()
    for n, shifts in enumerate(CHUNKS):
        bufs = [b for s in shifts for b in (own[s], partner[s])]
        last = n == len(CHUNKS) - 1
        state = attend_chunk(
            place, bufs, queries_t, state, shifts, y_count, 4, n == 0, last
        )
    arrived = along_x(state[0])

    mix_own = combine(arrived, query_blocks, newest_t, heads_dev)
    mix_partner = to_other_core(mix_own)
    partial = project(place, mix_own, mix_partner, out_weight, weight_partner, y_count)
    same_core = [[2 * i + c for i in range(y_count)] for c in range(2)]
    arrived = lax.all_to_all(partial, "tp", split_axis=0, concat_axis=0, axis_index_groups=same_core, tiled=True)
    return jnp.sum(arrived.astype(jnp.float32), axis=0).astype(jnp.bfloat16)


def solution(mesh):
    in_specs = (
        P(("rep", "grp"), "tp"),
        P(("rep", "grp"), None, None),
        P(("rep", "grp", "tp"), None, None, None),
        P("rep", ("grp", "tp"), None),
        P(("rep", "grp"), None),
        P(("rep", "grp")),
        P("tp", None),
    )
    out_specs = P(("rep", "grp"), "tp")
    return jax.shard_map(per_device_inner, mesh=mesh, in_specs=in_specs, out_specs=out_specs, check_vma=False)
```

```python
import math

import jax
import jax.numpy as jnp
from jax import lax
from jax.experimental import pallas as pl
from jax.experimental.pallas import tpu as pltpu
from jax.sharding import PartitionSpec as P

HEAD_SIZE = 128
PAGE_TOKENS = 128
META_ROWS = 16
NAMED_ROW = 10
LOW = -1e30
CHUNKS = ((0, 1, 7, 2, 6), (3, 5, 4))
STAT_ROWS = 16
INTERPRET = False
GRANT = 24 * 1024 * 1024


def split3(x):
    hi = x.astype(jnp.bfloat16)
    rest = x - hi.astype(jnp.float32)
    mid = rest.astype(jnp.bfloat16)
    low = (rest - mid.astype(jnp.float32)).astype(jnp.bfloat16)
    return [part.astype(jnp.float32) for part in (hi, mid, low)]


def prepare(queries, block_table, prefix_len, heads_dev, slots):
    req_rows = queries.shape[0]
    list_length = block_table.shape[1]
    cols = heads_dev * req_rows
    assert slots == cols

    def kernel(q_ref, table_ref, length_ref, out_ref):
        for h in range(heads_dev):
            one = q_ref[:, h * HEAD_SIZE : (h + 1) * HEAD_SIZE].astype(jnp.float32)
            out_ref[0:HEAD_SIZE, h * req_rows : (h + 1) * req_rows] = one.T.astype(jnp.bfloat16)
        length = length_ref[...]
        high = lax.div(length, 8)
        small = jnp.concatenate([table_ref[...], high, length - 8 * high, length], axis=0).astype(jnp.float32)
        small = jnp.concatenate([small, jnp.zeros((HEAD_SIZE - list_length - 3, req_rows), jnp.float32)], axis=0)
        lists = small.T
        slot = lax.broadcasted_iota(jnp.int32, (req_rows, slots), 1).astype(jnp.float32)
        hit = jnp.zeros((req_rows, slots), jnp.float32)
        for j in range(list_length):
            entry = jnp.where(lists[:, list_length + 2 : list_length + 3] > PAGE_TOKENS * j, lists[:, j : j + 1], -1.0)
            hit = jnp.where(slot == entry, 1.0, hit)
        named = jnp.max(hit, axis=0, keepdims=True)
        small = jnp.concatenate([small[0:META_ROWS]] * heads_dev, axis=1)
        sub = lax.broadcasted_iota(jnp.int32, (META_ROWS, cols), 0)
        out_ref[HEAD_SIZE:] = jnp.where(sub == list_length + 2, named, small).astype(jnp.bfloat16)

    return pl.pallas_call(
        kernel,
        out_shape=jax.ShapeDtypeStruct((HEAD_SIZE + META_ROWS, cols), jnp.bfloat16),
        interpret=INTERPRET,
        name="prepare",
    )(queries, block_table.T, prefix_len.reshape(1, -1))


def attend_chunk(place, bufs, queries_t, state, shifts, y_count, group_count, per_batch, first, last, early):
    n_buf = len(bufs)
    buf_rows = bufs[0].shape[0]
    rows, cols = queries_t[0].shape
    limit = 2 * n_buf
    factor = math.log2(math.e) / math.sqrt(HEAD_SIZE)
    int_rows = group_count + 8 * ((n_buf + 7) // 8)

    def kernel(place_ref, *refs):
        refs = refs[len(early) :]
        buf_refs = refs[:n_buf]
        q_refs = refs[n_buf : n_buf + group_count]
        rest = list(refs[n_buf + group_count :])
        if not first:
            acc_in, ml_in = rest[:2]
            rest = rest[2:]
        if last:
            out_ref = rest[0]
            rest = rest[1:]
        else:
            acc_out, ml_out = rest[:2]
            rest = rest[2:]
        (acc, ml, store, query_all, out_all, ints, numbers, item_row, item_slot, sem_store, sem_query, sem_acc, sem_ml, sem_int, sem_out) = rest
        tp_rank = place_ref[0]
        row = place_ref[1]
        core = lax.rem(tp_rank, 2)

        query_copies = [pltpu.make_async_copy(q_refs[g], query_all.at[g], sem_query.at[g]) for g in range(group_count)]
        store_copies = [
            pltpu.make_async_copy(buf_refs[b], store.at[pl.ds(b * buf_rows, buf_rows)], sem_store.at[b]) for b in range(n_buf)
        ]
        for one in query_copies + store_copies:
            one.start()
        if first:
            acc[...] = jnp.zeros(acc.shape, jnp.float32)
            ml[...] = jnp.where(lax.broadcasted_iota(jnp.int32, ml.shape, 1) == 0, LOW, 0.0)
        else:
            ml_copy = pltpu.make_async_copy(ml_in, ml, sem_ml)
            ml_copy.start()
            for g in range(group_count):
                pltpu.make_async_copy(acc_in.at[g], acc.at[g], sem_acc.at[g]).start()
        for one in query_copies + store_copies:
            one.wait()
        for g in range(group_count):
            ints[g : g + 1] = query_all[g, HEAD_SIZE:].astype(jnp.float32)[NAMED_ROW : NAMED_ROW + 1].astype(jnp.int32)
        for b in range(n_buf):
            pages = store[(b + 1) * buf_rows - META_ROWS : (b + 1) * buf_rows].astype(jnp.float32)
            ints[group_count + b : group_count + b + 1, 0:HEAD_SIZE] = pages[0:1].astype(jnp.int32)
        int_copy = pltpu.make_async_copy(ints, numbers, sem_int)
        int_copy.start()
        int_copy.wait()
        if not first:
            ml_copy.wait()

        entry = lax.broadcasted_iota(jnp.int32, (8, cols), 0).astype(jnp.float32)
        token = lax.broadcasted_iota(jnp.int32, (PAGE_TOKENS, cols), 0).astype(jnp.float32)

        def group(g, _):
            number = lax.rem(row + group_count - g, group_count)
            count = jnp.int32(0)
            for b in range(n_buf):
                source_y = lax.rem(lax.div(tp_rank, 2) + y_count - shifts[b // 2], y_count)
                owner = 2 * source_y + (core if b % 2 == 0 else 1 - core)
                for column in range(2):
                    page = numbers[group_count + b, 2 * number + column]
                    slot = (row * 2 * y_count + owner) * 2 + column
                    used = numbers[g, slot]
                    item_row[count] = b * buf_rows + page * (2 * PAGE_TOKENS)
                    item_slot[count] = slot
                    count = count + jnp.where((page >= 0) & (used > 0), 1, 0)
            for pad in range(per_batch):
                item_row[count + pad] = 0
                item_slot[count + pad] = -1

            table = query_all[g, HEAD_SIZE:].astype(jnp.float32)
            length = table[8:9] * 8.0 + table[9:10]
            table = table[0:8]
            live = jnp.clip(length - PAGE_TOKENS * entry, 0.0, 1.0 * PAGE_TOKENS)
            whole = live == PAGE_TOKENS
            if not first:
                pltpu.make_async_copy(acc_in.at[g], acc.at[g], sem_acc.at[g]).wait()

            def batch(i, _):
                query = query_all[g, 0:HEAD_SIZE]
                starts = [pl.multiple_of(item_row[i * per_batch + j], META_ROWS) for j in range(per_batch)]
                keys = jnp.concatenate([store[pl.ds(start, PAGE_TOKENS)] for start in starts], axis=0)
                raw = jnp.dot(keys, query, preferred_element_type=jnp.float32)
                old = ml[g, 0:1]
                top = old
                scores, counts = [], []
                for j in range(per_batch):
                    slot = item_slot[i * per_batch + j].astype(jnp.float32)
                    match = table == slot
                    full = jnp.sum(jnp.where(match & whole, 1.0, 0.0), axis=0, keepdims=True)
                    part = jnp.max(jnp.where(match & ~whole, live, 0.0), axis=0, keepdims=True)
                    reach = jnp.where(full > 0.0, 1.0 * PAGE_TOKENS, part)
                    score = raw[j * PAGE_TOKENS : (j + 1) * PAGE_TOKENS] * factor
                    score = jnp.where(token < reach, score, LOW)
                    top = jnp.maximum(top, jnp.max(score, axis=0, keepdims=True))
                    scores.append(score)
                    counts.append((full, part))
                shrink = jnp.exp2(old - top)
                total = ml[g, 1:2] * shrink
                weights = []
                for j in range(per_batch):
                    full, part = counts[j]
                    weight = jnp.exp2(scores[j] - top) * jnp.where(token < part, full + 1.0, full)
                    total = total + jnp.sum(weight, axis=0, keepdims=True)
                    weights.append(weight.astype(jnp.bfloat16))
                values = jnp.concatenate([store[pl.ds(start + PAGE_TOKENS, PAGE_TOKENS)] for start in starts], axis=0)
                added = lax.dot_general(
                    values, jnp.concatenate(weights, axis=0), (((0,), (0,)), ((), ())), preferred_element_type=jnp.float32
                )
                acc[g] = acc[g] * shrink + added
                ml[g, 0:1] = top
                ml[g, 1:2] = total
                return 0

            lax.fori_loop(0, lax.div(count + per_batch - 1, per_batch), batch, 0)

            if last:
                top = ml[g, 0:1]
                total = ml[g, 1:2]
                inverse = jnp.where(total > 0.0, 1.0 / jnp.where(total > 0.0, total, 1.0), 0.0)
                out_all[g, 0:HEAD_SIZE] = (acc[g] * inverse).astype(jnp.bfloat16)
                sub = lax.broadcasted_iota(jnp.int32, (STAT_ROWS, cols), 0)
                packed = jnp.zeros((STAT_ROWS, cols), jnp.float32)
                for n, part in enumerate(split3(top) + split3(total)):
                    packed = jnp.where(sub == n, part, packed)
                out_all[g, HEAD_SIZE:] = packed.astype(jnp.bfloat16)
                pltpu.make_async_copy(out_all.at[g], out_ref.at[number], sem_out.at[g]).start()
            else:
                pltpu.make_async_copy(acc.at[g], acc_out.at[g], sem_out.at[g]).start()
            return 0

        lax.fori_loop(0, group_count, group, 0)
        if last:
            for n in range(group_count):
                pltpu.make_async_copy(out_all.at[n], out_ref.at[n], sem_out.at[n]).wait()
        else:
            ml_back = pltpu.make_async_copy(ml, ml_out, sem_ml)
            ml_back.start()
            for n in range(group_count):
                pltpu.make_async_copy(acc.at[n], acc_out.at[n], sem_out.at[n]).wait()
            ml_back.wait()

    if last:
        out_shape = [jax.ShapeDtypeStruct((group_count, HEAD_SIZE + STAT_ROWS, cols), jnp.bfloat16)]
    else:
        out_shape = [
            jax.ShapeDtypeStruct((group_count, HEAD_SIZE, cols), jnp.float32),
            jax.ShapeDtypeStruct((group_count, 8, cols), jnp.float32),
        ]
    n_out_slots = group_count if last else 1
    scratch = [
        pltpu.VMEM((group_count, HEAD_SIZE, cols), jnp.float32),
        pltpu.VMEM((group_count, 8, cols), jnp.float32),
        pltpu.VMEM((n_buf * buf_rows, HEAD_SIZE), jnp.bfloat16),
        pltpu.VMEM((group_count, rows, cols), jnp.bfloat16),
        pltpu.VMEM((n_out_slots, HEAD_SIZE + STAT_ROWS, cols), jnp.bfloat16),
        pltpu.VMEM((int_rows, cols), jnp.int32),
        pltpu.SMEM((int_rows, cols), jnp.int32),
        pltpu.SMEM((limit + per_batch,), jnp.int32),
        pltpu.SMEM((limit + per_batch,), jnp.int32),
        pltpu.SemaphoreType.DMA((n_buf,)),
        pltpu.SemaphoreType.DMA((group_count,)),
        pltpu.SemaphoreType.DMA((group_count,)),
        pltpu.SemaphoreType.DMA,
        pltpu.SemaphoreType.DMA,
        pltpu.SemaphoreType.DMA((group_count,)),
    ]
    anywhere = pl.BlockSpec(memory_space=pltpu.MemorySpace.HBM)
    n_in = len(early) + n_buf + group_count + (0 if first else 2)
    return pl.pallas_call(
        kernel,
        out_shape=out_shape,
        grid_spec=pltpu.PrefetchScalarGridSpec(
            num_scalar_prefetch=1,
            grid=(),
            in_specs=[anywhere] * n_in,
            out_specs=[anywhere] * len(out_shape),
            scratch_shapes=scratch,
        ),
        interpret=INTERPRET,
    )(place, *early, *bufs, *queries_t, *(() if first else state))


def combine(arrived, query_t, newest_t, heads_dev):
    parts, _, cols = arrived.shape
    req_rows = cols // heads_dev
    factor = math.log2(math.e) / math.sqrt(HEAD_SIZE)

    def kernel(in_ref, q_ref, new_ref, out_ref):
        query = q_ref[0:HEAD_SIZE].astype(jnp.float32)
        own = jnp.sum(query * new_ref[0].astype(jnp.float32), axis=0, keepdims=True) * factor
        top = own
        tops, totals = [], []
        for n in range(parts):
            packed = in_ref[n, HEAD_SIZE:].astype(jnp.float32)
            tops.append(packed[0:1] + packed[1:2] + packed[2:3])
            totals.append(packed[3:4] + packed[4:5] + packed[5:6])
            top = jnp.maximum(top, tops[-1])
        own_weight = jnp.exp2(own - top)
        denominator = own_weight
        scales = []
        for n in range(parts):
            scales.append(totals[n] * jnp.exp2(tops[n] - top))
            denominator = denominator + scales[-1]
        inverse = 1.0 / denominator
        mix = new_ref[1].astype(jnp.float32) * (own_weight * inverse)
        for n in range(parts):
            mix = mix + in_ref[n, 0:HEAD_SIZE].astype(jnp.float32) * (scales[n] * inverse)
        for h in range(heads_dev):
            one = mix[:, h * req_rows : (h + 1) * req_rows]
            out_ref[:, h * HEAD_SIZE : (h + 1) * HEAD_SIZE] = one.T.astype(jnp.bfloat16)

    return pl.pallas_call(
        kernel,
        out_shape=jax.ShapeDtypeStruct((req_rows, heads_dev * HEAD_SIZE), jnp.bfloat16),
        interpret=INTERPRET,
        compiler_params=pltpu.CompilerParams(vmem_limit_bytes=GRANT),
        name="combine",
    )(arrived, query_t, newest_t)


def held_weights(place, weight_own, weight_partner, y_count):
    width = weight_own.shape[1] // (2 * y_count)
    depth = weight_own.shape[0]

    def kernel(place_ref, w_own_ref, w_partner_ref, out_ref, sem):
        core = lax.rem(place_ref[0], 2)
        copies = []
        for n in range(y_count):
            start = pl.multiple_of((2 * n + core) * width, width)
            for k, ref in enumerate((w_own_ref, w_partner_ref)):
                copies.append(
                    pltpu.make_async_copy(
                        ref.at[:, pl.ds(start, width)], out_ref.at[n, pl.ds(k * depth, depth)], sem.at[2 * n + k]
                    )
                )
        for one in copies:
            one.start()
        for one in copies:
            one.wait()

    anywhere = pl.BlockSpec(memory_space=pltpu.MemorySpace.HBM)
    return pl.pallas_call(
        kernel,
        out_shape=pltpu.VMEM((y_count, 2 * depth, width), jnp.bfloat16),
        grid_spec=pltpu.PrefetchScalarGridSpec(
            num_scalar_prefetch=1,
            grid=(),
            in_specs=[anywhere, anywhere],
            out_specs=pl.BlockSpec(memory_space=pltpu.MemorySpace.VMEM),
            scratch_shapes=[pltpu.SemaphoreType.DMA((2 * y_count,))],
        ),
        interpret=INTERPRET,
        compiler_params=pltpu.CompilerParams(vmem_limit_bytes=GRANT),
        name="held_weights",
    )(place, weight_own, weight_partner)


def project(mix_own, mix_partner, weights):
    y_count, _, width = weights.shape
    req_rows, _ = mix_own.shape

    def kernel(own_ref, partner_ref, w_ref, out_ref):
        mix = jnp.concatenate([own_ref[...], partner_ref[...]], axis=1)
        for n in range(y_count):
            out_ref[n] = jnp.dot(mix, w_ref[n], preferred_element_type=jnp.float32).astype(jnp.bfloat16)

    vmem = pl.BlockSpec(memory_space=pltpu.MemorySpace.VMEM)
    return pl.pallas_call(
        kernel,
        out_shape=jax.ShapeDtypeStruct((y_count, req_rows, width), jnp.bfloat16),
        in_specs=[vmem, vmem, vmem],
        out_specs=vmem,
        interpret=INTERPRET,
        compiler_params=pltpu.CompilerParams(vmem_limit_bytes=GRANT),
        name="project",
    )(mix_own, mix_partner, weights)


def per_device_inner(
    queries, newest_key_value, kv_pages, fetch_slots, block_table, prefix_len, out_weight
):
    tp_count = lax.axis_size("tp")
    group_count = lax.axis_size("grp")
    y_count = tp_count // 2
    tp_rank = lax.axis_index("tp").astype(jnp.int32)
    row = lax.axis_index("grp").astype(jnp.int32)
    y = lax.div(tp_rank, 2)
    heads_dev = queries.shape[1] // HEAD_SIZE
    slots = 2 * tp_count * group_count
    swap = [(i, i ^ 1) for i in range(tp_count)]

    def along_y(x, shift):
        return lax.ppermute(x, "tp", [(i, (i + 2 * shift) % tp_count) for i in range(tp_count)])

    def along_x(x, shift):
        return lax.ppermute(x, "grp", [(i, (i + shift) % group_count) for i in range(group_count)])

    def to_other_core(x):
        return lax.ppermute(x, "tp", swap)

    slots_block = jnp.pad(fetch_slots.reshape(1, -1).astype(jnp.bfloat16), ((0, META_ROWS - 1), (0, HEAD_SIZE - 2 * group_count)))
    own, partner = {}, {}
    for shift in [s for chunk in CHUNKS for s in chunk]:
        head = lax.rem(y + shift, y_count)
        piece = lax.dynamic_slice_in_dim(kv_pages, head * HEAD_SIZE, HEAD_SIZE, 3)
        piece = jnp.concatenate([piece.reshape(-1, HEAD_SIZE), slots_block], axis=0)
        own[shift] = along_y(piece, shift) if shift else piece
    for shift in own:
        partner[shift] = to_other_core(own[shift])
    weight_partner = to_other_core(out_weight)

    query_t = prepare(queries, block_table, prefix_len, heads_dev, slots)
    queries_t = [along_x(query_t, s) if s else query_t for s in range(group_count)]
    place = jnp.stack([tp_rank, row])

    newest = lax.dynamic_slice_in_dim(newest_key_value, y * HEAD_SIZE, HEAD_SIZE, 2)
    newest_t = jnp.tile(jnp.transpose(newest, (1, 2, 0)), (1, 1, heads_dev))

    state = ()
    for n, shifts in enumerate(CHUNKS):
        bufs = [b for s in shifts for b in (own[s], partner[s])]
        last = n == len(CHUNKS) - 1
        state = attend_chunk(
            place, bufs, queries_t, state, shifts, y_count, group_count, 4, n == 0, last, (newest_t,) if last else ()
        )
    arrived = lax.all_to_all(state[0], "grp", split_axis=0, concat_axis=0, tiled=True)
    weights = held_weights(place, out_weight, weight_partner, y_count)

    mix_own = combine(arrived, query_t, newest_t, heads_dev)
    mix_partner = to_other_core(mix_own)
    partial = project(mix_own, mix_partner, weights)
    same_core = [[2 * i + c for i in range(y_count)] for c in range(2)]
    arrived = lax.all_to_all(partial, "tp", split_axis=0, concat_axis=0, axis_index_groups=same_core, tiled=True)
    return jnp.sum(arrived.astype(jnp.float32), axis=0).astype(jnp.bfloat16)


def solution(mesh):
    in_specs = (
        P(("rep", "grp"), "tp"),
        P(("rep", "grp"), None, None),
        P(("rep", "grp", "tp"), None, None, None),
        P("rep", ("grp", "tp"), None),
        P(("rep", "grp"), None),
        P(("rep", "grp")),
        P("tp", None),
    )
    out_specs = P(("rep", "grp"), "tp")
    return jax.shard_map(per_device_inner, mesh=mesh, in_specs=in_specs, out_specs=out_specs, check_vma=False)
```

```python
import math

import jax
import jax.numpy as jnp
from jax import lax
from jax.experimental import pallas as pl
from jax.experimental.pallas import tpu as pltpu
from jax.sharding import PartitionSpec as P

HEAD_SIZE = 128
PAGE_TOKENS = 128
META_ROWS = 16
NAMED_ROW = 10
LOW = -1e30
CHUNKS = ((0, 1, 7, 2, 6), (3, 5, 4))
STAT_ROWS = 16
INTERPRET = False
GRANT = 24 * 1024 * 1024


def split3(x):
    hi = x.astype(jnp.bfloat16)
    rest = x - hi.astype(jnp.float32)
    mid = rest.astype(jnp.bfloat16)
    low = (rest - mid.astype(jnp.float32)).astype(jnp.bfloat16)
    return [part.astype(jnp.float32) for part in (hi, mid, low)]


def prepare(queries, block_table, prefix_len, heads_dev, slots):
    req_rows = queries.shape[0]
    list_length = block_table.shape[1]
    cols = heads_dev * req_rows
    assert slots == cols

    def kernel(q_ref, table_ref, length_ref, out_ref):
        for h in range(heads_dev):
            one = q_ref[:, h * HEAD_SIZE : (h + 1) * HEAD_SIZE].astype(jnp.float32)
            out_ref[0:HEAD_SIZE, h * req_rows : (h + 1) * req_rows] = one.T.astype(jnp.bfloat16)
        length = length_ref[...]
        high = lax.div(length, 8)
        small = jnp.concatenate([table_ref[...], high, length - 8 * high, length], axis=0).astype(jnp.float32)
        small = jnp.concatenate([small, jnp.zeros((HEAD_SIZE - list_length - 3, req_rows), jnp.float32)], axis=0)
        lists = small.T
        slot = lax.broadcasted_iota(jnp.int32, (req_rows, slots), 1).astype(jnp.float32)
        hit = jnp.zeros((req_rows, slots), jnp.float32)
        for j in range(list_length):
            entry = jnp.where(lists[:, list_length + 2 : list_length + 3] > PAGE_TOKENS * j, lists[:, j : j + 1], -1.0)
            hit = jnp.where(slot == entry, 1.0, hit)
        named = jnp.max(hit, axis=0, keepdims=True)
        small = jnp.concatenate([small[0:META_ROWS]] * heads_dev, axis=1)
        sub = lax.broadcasted_iota(jnp.int32, (META_ROWS, cols), 0)
        out_ref[HEAD_SIZE:] = jnp.where(sub == list_length + 2, named, small).astype(jnp.bfloat16)

    return pl.pallas_call(
        kernel,
        out_shape=jax.ShapeDtypeStruct((HEAD_SIZE + META_ROWS, cols), jnp.bfloat16),
        interpret=INTERPRET,
        name="prepare",
    )(queries, block_table.T, prefix_len.reshape(1, -1))


def attend_chunk(place, bufs, queries_t, state, shifts, y_count, group_count, per_batch, first, last, early):
    n_buf = len(bufs)
    buf_rows = bufs[0].shape[0]
    rows, cols = queries_t[0].shape
    limit = 2 * n_buf
    factor = math.log2(math.e) / math.sqrt(HEAD_SIZE)
    int_rows = group_count + 8 * ((n_buf + 7) // 8)

    def kernel(place_ref, *refs):
        refs = refs[len(early) :]
        buf_refs = refs[:n_buf]
        q_refs = refs[n_buf : n_buf + group_count]
        rest = list(refs[n_buf + group_count :])
        if not first:
            acc_in, ml_in = rest[:2]
            rest = rest[2:]
        if last:
            out_ref = rest[0]
            rest = rest[1:]
        else:
            acc_out, ml_out = rest[:2]
            rest = rest[2:]
        (acc, ml, store, query_all, out_all, ints, numbers, item_row, item_slot, sem_store, sem_query, sem_acc, sem_ml, sem_int, sem_out) = rest
        tp_rank = place_ref[0]
        row = place_ref[1]
        core = lax.rem(tp_rank, 2)

        query_copies = [pltpu.make_async_copy(q_refs[g], query_all.at[g], sem_query.at[g]) for g in range(group_count)]
        store_copies = [
            pltpu.make_async_copy(buf_refs[b], store.at[pl.ds(b * buf_rows, buf_rows)], sem_store.at[b]) for b in range(n_buf)
        ]
        for one in query_copies + store_copies:
            one.start()
        if first:
            acc[...] = jnp.zeros(acc.shape, jnp.float32)
            ml[...] = jnp.where(lax.broadcasted_iota(jnp.int32, ml.shape, 1) == 0, LOW, 0.0)
        else:
            ml_copy = pltpu.make_async_copy(ml_in, ml, sem_ml)
            ml_copy.start()
            for g in range(group_count):
                pltpu.make_async_copy(acc_in.at[g], acc.at[g], sem_acc.at[g]).start()
        for one in query_copies + store_copies:
            one.wait()
        for g in range(group_count):
            ints[g : g + 1] = query_all[g, HEAD_SIZE:].astype(jnp.float32)[NAMED_ROW : NAMED_ROW + 1].astype(jnp.int32)
        for b in range(n_buf):
            pages = store[(b + 1) * buf_rows - META_ROWS : (b + 1) * buf_rows].astype(jnp.float32)
            ints[group_count + b : group_count + b + 1, 0:HEAD_SIZE] = pages[0:1].astype(jnp.int32)
        int_copy = pltpu.make_async_copy(ints, numbers, sem_int)
        int_copy.start()
        int_copy.wait()
        if not first:
            ml_copy.wait()

        entry = lax.broadcasted_iota(jnp.int32, (8, cols), 0).astype(jnp.float32)
        token = lax.broadcasted_iota(jnp.int32, (PAGE_TOKENS, cols), 0).astype(jnp.float32)

        def group(g, _):
            number = lax.rem(row + group_count - g, group_count)
            count = jnp.int32(0)
            for b in range(n_buf):
                source_y = lax.rem(lax.div(tp_rank, 2) + y_count - shifts[b // 2], y_count)
                owner = 2 * source_y + (core if b % 2 == 0 else 1 - core)
                for column in range(2):
                    page = numbers[group_count + b, 2 * number + column]
                    slot = (row * 2 * y_count + owner) * 2 + column
                    used = numbers[g, slot]
                    item_row[count] = b * buf_rows + page * (2 * PAGE_TOKENS)
                    item_slot[count] = slot
                    count = count + jnp.where((page >= 0) & (used > 0), 1, 0)
            for pad in range(per_batch):
                item_row[count + pad] = 0
                item_slot[count + pad] = -1

            table = query_all[g, HEAD_SIZE:].astype(jnp.float32)
            length = table[8:9] * 8.0 + table[9:10]
            table = table[0:8]
            live = jnp.clip(length - PAGE_TOKENS * entry, 0.0, 1.0 * PAGE_TOKENS)
            whole = live == PAGE_TOKENS
            if not first:
                pltpu.make_async_copy(acc_in.at[g], acc.at[g], sem_acc.at[g]).wait()

            def batch(i, _):
                query = query_all[g, 0:HEAD_SIZE]
                starts = [pl.multiple_of(item_row[i * per_batch + j], META_ROWS) for j in range(per_batch)]
                keys = jnp.concatenate([store[pl.ds(start, PAGE_TOKENS)] for start in starts], axis=0)
                raw = jnp.dot(keys, query, preferred_element_type=jnp.float32)
                old = ml[g, 0:1]
                top = old
                scores, counts = [], []
                for j in range(per_batch):
                    slot = item_slot[i * per_batch + j].astype(jnp.float32)
                    match = table == slot
                    full = jnp.sum(jnp.where(match & whole, 1.0, 0.0), axis=0, keepdims=True)
                    part = jnp.max(jnp.where(match & ~whole, live, 0.0), axis=0, keepdims=True)
                    reach = jnp.where(full > 0.0, 1.0 * PAGE_TOKENS, part)
                    score = raw[j * PAGE_TOKENS : (j + 1) * PAGE_TOKENS] * factor
                    score = jnp.where(token < reach, score, LOW)
                    top = jnp.maximum(top, jnp.max(score, axis=0, keepdims=True))
                    scores.append(score)
                    counts.append((full, part))
                shrink = jnp.exp2(old - top)
                total = ml[g, 1:2] * shrink
                weights = []
                for j in range(per_batch):
                    full, part = counts[j]
                    weight = jnp.exp2(scores[j] - top) * jnp.where(token < part, full + 1.0, full)
                    total = total + jnp.sum(weight, axis=0, keepdims=True)
                    weights.append(weight.astype(jnp.bfloat16))
                values = jnp.concatenate([store[pl.ds(start + PAGE_TOKENS, PAGE_TOKENS)] for start in starts], axis=0)
                added = lax.dot_general(
                    values, jnp.concatenate(weights, axis=0), (((0,), (0,)), ((), ())), preferred_element_type=jnp.float32
                )
                acc[g] = acc[g] * shrink + added
                ml[g, 0:1] = top
                ml[g, 1:2] = total
                return 0

            lax.fori_loop(0, lax.div(count + per_batch - 1, per_batch), batch, 0)

            if last:
                top = ml[g, 0:1]
                total = ml[g, 1:2]
                inverse = jnp.where(total > 0.0, 1.0 / jnp.where(total > 0.0, total, 1.0), 0.0)
                out_all[g, 0:HEAD_SIZE] = (acc[g] * inverse).astype(jnp.bfloat16)
                sub = lax.broadcasted_iota(jnp.int32, (STAT_ROWS, cols), 0)
                packed = jnp.zeros((STAT_ROWS, cols), jnp.float32)
                for n, part in enumerate(split3(top) + split3(total)):
                    packed = jnp.where(sub == n, part, packed)
                out_all[g, HEAD_SIZE:] = packed.astype(jnp.bfloat16)
                pltpu.make_async_copy(out_all.at[g], out_ref.at[number], sem_out.at[g]).start()
            else:
                pltpu.make_async_copy(acc.at[g], acc_out.at[g], sem_out.at[g]).start()
            return 0

        lax.fori_loop(0, group_count, group, 0)
        if last:
            for n in range(group_count):
                pltpu.make_async_copy(out_all.at[n], out_ref.at[n], sem_out.at[n]).wait()
        else:
            ml_back = pltpu.make_async_copy(ml, ml_out, sem_ml)
            ml_back.start()
            for n in range(group_count):
                pltpu.make_async_copy(acc.at[n], acc_out.at[n], sem_out.at[n]).wait()
            ml_back.wait()

    if last:
        out_shape = [jax.ShapeDtypeStruct((group_count, HEAD_SIZE + STAT_ROWS, cols), jnp.bfloat16)]
    else:
        out_shape = [
            jax.ShapeDtypeStruct((group_count, HEAD_SIZE, cols), jnp.float32),
            jax.ShapeDtypeStruct((group_count, 8, cols), jnp.float32),
        ]
    n_out_slots = group_count if last else 1
    scratch = [
        pltpu.VMEM((group_count, HEAD_SIZE, cols), jnp.float32),
        pltpu.VMEM((group_count, 8, cols), jnp.float32),
        pltpu.VMEM((n_buf * buf_rows, HEAD_SIZE), jnp.bfloat16),
        pltpu.VMEM((group_count, rows, cols), jnp.bfloat16),
        pltpu.VMEM((n_out_slots, HEAD_SIZE + STAT_ROWS, cols), jnp.bfloat16),
        pltpu.VMEM((int_rows, cols), jnp.int32),
        pltpu.SMEM((int_rows, cols), jnp.int32),
        pltpu.SMEM((limit + per_batch,), jnp.int32),
        pltpu.SMEM((limit + per_batch,), jnp.int32),
        pltpu.SemaphoreType.DMA((n_buf,)),
        pltpu.SemaphoreType.DMA((group_count,)),
        pltpu.SemaphoreType.DMA((group_count,)),
        pltpu.SemaphoreType.DMA,
        pltpu.SemaphoreType.DMA,
        pltpu.SemaphoreType.DMA((group_count,)),
    ]
    anywhere = pl.BlockSpec(memory_space=pltpu.MemorySpace.HBM)
    n_in = len(early) + n_buf + group_count + (0 if first else 2)
    return pl.pallas_call(
        kernel,
        out_shape=out_shape,
        grid_spec=pltpu.PrefetchScalarGridSpec(
            num_scalar_prefetch=1,
            grid=(),
            in_specs=[anywhere] * n_in,
            out_specs=[anywhere] * len(out_shape),
            scratch_shapes=scratch,
        ),
        interpret=INTERPRET,
    )(place, *early, *bufs, *queries_t, *(() if first else state))


def combine(place, arrived, query_t, newest_t, weight_own, weight_partner, heads_dev, y_count):
    width = weight_own.shape[1] // (2 * y_count)
    depth = weight_own.shape[0]
    parts, _, cols = arrived.shape
    req_rows = cols // heads_dev
    factor = math.log2(math.e) / math.sqrt(HEAD_SIZE)

    def kernel(place_ref, in_ref, q_ref, new_ref, w_own_ref, w_partner_ref, out_ref, held_ref, sem):
        core = lax.rem(place_ref[0], 2)
        copies = []
        for n in range(y_count):
            start = pl.multiple_of((2 * n + core) * width, width)
            for k, ref in enumerate((w_own_ref, w_partner_ref)):
                copies.append(
                    pltpu.make_async_copy(
                        ref.at[:, pl.ds(start, width)], held_ref.at[n, pl.ds(k * depth, depth)], sem.at[2 * n + k]
                    )
                )
        for one in copies:
            one.start()
        query = q_ref[0:HEAD_SIZE].astype(jnp.float32)
        own = jnp.sum(query * new_ref[0].astype(jnp.float32), axis=0, keepdims=True) * factor
        top = own
        tops, totals = [], []
        for n in range(parts):
            packed = in_ref[n, HEAD_SIZE:].astype(jnp.float32)
            tops.append(packed[0:1] + packed[1:2] + packed[2:3])
            totals.append(packed[3:4] + packed[4:5] + packed[5:6])
            top = jnp.maximum(top, tops[-1])
        own_weight = jnp.exp2(own - top)
        denominator = own_weight
        scales = []
        for n in range(parts):
            scales.append(totals[n] * jnp.exp2(tops[n] - top))
            denominator = denominator + scales[-1]
        inverse = 1.0 / denominator
        mix = new_ref[1].astype(jnp.float32) * (own_weight * inverse)
        for n in range(parts):
            mix = mix + in_ref[n, 0:HEAD_SIZE].astype(jnp.float32) * (scales[n] * inverse)
        for h in range(heads_dev):
            one = mix[:, h * req_rows : (h + 1) * req_rows]
            out_ref[:, h * HEAD_SIZE : (h + 1) * HEAD_SIZE] = one.T.astype(jnp.bfloat16)
        for one in copies:
            one.wait()

    vmem = pl.BlockSpec(memory_space=pltpu.MemorySpace.VMEM)
    anywhere = pl.BlockSpec(memory_space=pltpu.MemorySpace.HBM)
    return pl.pallas_call(
        kernel,
        out_shape=[
            jax.ShapeDtypeStruct((req_rows, heads_dev * HEAD_SIZE), jnp.bfloat16),
            pltpu.VMEM((y_count, 2 * depth, width), jnp.bfloat16),
        ],
        grid_spec=pltpu.PrefetchScalarGridSpec(
            num_scalar_prefetch=1,
            grid=(),
            in_specs=[vmem, vmem, vmem, anywhere, anywhere],
            out_specs=[vmem, vmem],
            scratch_shapes=[pltpu.SemaphoreType.DMA((2 * y_count,))],
        ),
        interpret=INTERPRET,
        compiler_params=pltpu.CompilerParams(vmem_limit_bytes=GRANT),
        name="combine",
    )(place, arrived, query_t, newest_t, weight_own, weight_partner)


def project(mix_own, mix_partner, weights):
    y_count, _, width = weights.shape
    req_rows, _ = mix_own.shape

    def kernel(own_ref, partner_ref, w_ref, out_ref):
        mix = jnp.concatenate([own_ref[...], partner_ref[...]], axis=1)
        for n in range(y_count):
            out_ref[n] = jnp.dot(mix, w_ref[n], preferred_element_type=jnp.float32).astype(jnp.bfloat16)

    vmem = pl.BlockSpec(memory_space=pltpu.MemorySpace.VMEM)
    return pl.pallas_call(
        kernel,
        out_shape=jax.ShapeDtypeStruct((y_count, req_rows, width), jnp.bfloat16),
        in_specs=[vmem, vmem, vmem],
        out_specs=vmem,
        interpret=INTERPRET,
        compiler_params=pltpu.CompilerParams(vmem_limit_bytes=GRANT),
        name="project",
    )(mix_own, mix_partner, weights)


def per_device_inner(
    queries, newest_key_value, kv_pages, fetch_slots, block_table, prefix_len, out_weight
):
    tp_count = lax.axis_size("tp")
    group_count = lax.axis_size("grp")
    y_count = tp_count // 2
    tp_rank = lax.axis_index("tp").astype(jnp.int32)
    row = lax.axis_index("grp").astype(jnp.int32)
    y = lax.div(tp_rank, 2)
    heads_dev = queries.shape[1] // HEAD_SIZE
    slots = 2 * tp_count * group_count
    swap = [(i, i ^ 1) for i in range(tp_count)]

    def along_y(x, shift):
        return lax.ppermute(x, "tp", [(i, (i + 2 * shift) % tp_count) for i in range(tp_count)])

    def along_x(x, shift):
        return lax.ppermute(x, "grp", [(i, (i + shift) % group_count) for i in range(group_count)])

    def to_other_core(x):
        return lax.ppermute(x, "tp", swap)

    slots_block = jnp.pad(fetch_slots.reshape(1, -1).astype(jnp.bfloat16), ((0, META_ROWS - 1), (0, HEAD_SIZE - 2 * group_count)))
    own, partner = {}, {}
    for shift in [s for chunk in CHUNKS for s in chunk]:
        head = lax.rem(y + shift, y_count)
        piece = lax.dynamic_slice_in_dim(kv_pages, head * HEAD_SIZE, HEAD_SIZE, 3)
        piece = jnp.concatenate([piece.reshape(-1, HEAD_SIZE), slots_block], axis=0)
        own[shift] = along_y(piece, shift) if shift else piece
    for shift in own:
        partner[shift] = to_other_core(own[shift])
    weight_partner = to_other_core(out_weight)

    query_t = prepare(queries, block_table, prefix_len, heads_dev, slots)
    queries_t = [along_x(query_t, s) if s else query_t for s in range(group_count)]
    place = jnp.stack([tp_rank, row])

    newest = lax.dynamic_slice_in_dim(newest_key_value, y * HEAD_SIZE, HEAD_SIZE, 2)
    newest_t = jnp.tile(jnp.transpose(newest, (1, 2, 0)), (1, 1, heads_dev))

    state = ()
    for n, shifts in enumerate(CHUNKS):
        bufs = [b for s in shifts for b in (own[s], partner[s])]
        last = n == len(CHUNKS) - 1
        state = attend_chunk(
            place, bufs, queries_t, state, shifts, y_count, group_count, 4, n == 0, last, (newest_t,) if last else ()
        )
    arrived = lax.all_to_all(state[0], "grp", split_axis=0, concat_axis=0, tiled=True)

    mix_own, weights = combine(place, arrived, query_t, newest_t, out_weight, weight_partner, heads_dev, y_count)
    mix_partner = to_other_core(mix_own)
    partial = project(mix_own, mix_partner, weights)
    same_core = [[2 * i + c for i in range(y_count)] for c in range(2)]
    arrived = lax.all_to_all(partial, "tp", split_axis=0, concat_axis=0, axis_index_groups=same_core, tiled=True)
    return jnp.sum(arrived.astype(jnp.float32), axis=0).astype(jnp.bfloat16)


def solution(mesh):
    in_specs = (
        P(("rep", "grp"), "tp"),
        P(("rep", "grp"), None, None),
        P(("rep", "grp", "tp"), None, None, None),
        P("rep", ("grp", "tp"), None),
        P(("rep", "grp"), None),
        P(("rep", "grp")),
        P("tp", None),
    )
    out_specs = P(("rep", "grp"), "tp")
    return jax.shard_map(per_device_inner, mesh=mesh, in_specs=in_specs, out_specs=out_specs, check_vma=False)
```
